32 devices in a mesh: dp: 4 (over y, z), ep: 8 (over x, core).
Axes of the slice: x: 4, y: 2, z: 2, core: 2. Of those that a mesh axis runs over, the one named last changes fastest.
The devices are a block of a 4x4x8 slice.
Arguments:
- hidden: bfloat16 [2048, 2048], P(('dp', 'ep')), parts along dimension 0
- positions: int32 [2048], P(('dp', 'ep')), parts along dimension 0
- expert_ids: int32 [2, 2048, 8], P(None, ('dp', 'ep')), parts along dimension 1
- k_cache: bfloat16 [2, 2048, 16, 4, 128], P(None, ('dp', 'ep')), parts along dimension 1
- v_cache: bfloat16 [2, 2048, 16, 4, 128], P(None, ('dp', 'ep')), parts along dimension 1
- w_query: bfloat16 [2, 2048, 4096], replicated
- w_key: bfloat16 [2, 2048, 512], replicated
- w_value: bfloat16 [2, 2048, 512], replicated
- w_out: bfloat16 [2, 4096, 2048], replicated
- attn_gain: float32 [2, 2048], replicated
- q_gain: float32 [2, 4096], replicated
- k_gain: float32 [2, 512], replicated
- mlp_gain: float32 [2, 2048], replicated
- w_router: bfloat16 [2048, 128], replicated
- w_gate: bfloat16 [128, 2048, 768], P('ep')
- w_up: bfloat16 [128, 2048, 768], P('ep')
- w_down: bfloat16 [128, 768, 2048], P('ep')
Outputs:
- output 1: bfloat16 [2048, 2048], P(('dp', 'ep')), parts along dimension 0
- output 2: bfloat16 [2, 2048, 16, 4, 128], P(None, ('dp', 'ep')), parts along dimension 1
- output 3: bfloat16 [2, 2048, 16, 4, 128], P(None, ('dp', 'ep')), parts along dimension 1
There are 4 independent parts. The reference program is written for one: setup_inputs(seed, part) draws one part's arguments, and reference() takes and returns one part's arrays. A program takes and returns all parts, laid end to end along the dimension named above; an argument that names none is the same for every part.
All inputs are finite; a program needn't handle non-finite values.
Results may differ from the reference program's by a relative error of at most 0.02.
Values are sent between devices in bfloat16 or wider.
A program may use at most 768 MiB of HBM per device.

```python
import jax
import jax.numpy as jnp
from jax import lax

SEQ_COUNT = 512
CACHE_LEN = 16
MODEL_DIM = 2048
NUM_HEADS = 32
KV_HEADS = 4
HEAD_DIM = 128
NUM_EXPERTS = 128
TOP_K = 8
FFN_DIM = 768
EP_GROUPS = 8
NUM_LAYERS = 2

LOCAL_SEQS = SEQ_COUNT // EP_GROUPS
CAPACITY = 2 * LOCAL_SEQS * TOP_K // NUM_EXPERTS
WINDOWS = NUM_EXPERTS // TOP_K
Q_WIDTH = NUM_HEADS * HEAD_DIM
KV_WIDTH = KV_HEADS * HEAD_DIM
RMS_EPS = 1e-5
ROPE_BASE = 10000.0


def block_routes(rng_key):
    key_rows, key_perm = jax.random.split(rng_key)
    spread = jnp.arange(LOCAL_SEQS - CAPACITY, dtype=jnp.int32) % (WINDOWS - 1) + 1
    window_list = jnp.concatenate([jnp.zeros((CAPACITY,), jnp.int32), spread])
    windows = window_list[jax.random.permutation(key_rows, LOCAL_SEQS)]
    expert_perm = jax.random.permutation(key_perm, NUM_EXPERTS).astype(jnp.int32)
    slot_ids = windows[:, None] * TOP_K + jnp.arange(TOP_K, dtype=jnp.int32)[None, :]
    return expert_perm[slot_ids]


def draw_routes(rng_key):
    layer_keys = jax.random.split(rng_key, NUM_LAYERS * EP_GROUPS)
    routes = jax.vmap(block_routes)(layer_keys)
    return routes.reshape(NUM_LAYERS, SEQ_COUNT, TOP_K)


def draw_positions(rng_key):
    key_len, key_top = jax.random.split(rng_key)
    positions = jax.random.randint(key_len, (SEQ_COUNT,), 0, CACHE_LEN, dtype=jnp.int32)
    longest = jax.random.randint(key_top, (), 0, SEQ_COUNT)
    return positions.at[longest].set(CACHE_LEN - 1)


def setup_inputs(seed: int = 0, part: int = 0) -> dict:
    part_keys = jax.random.split(jax.random.fold_in(jax.random.key(seed + 1), part), 5)
    shared = jax.random.split(jax.random.key(seed), 12)

    def draw_normal(rng_key, shape, scale):
        return (jax.random.normal(rng_key, shape, jnp.float32) * scale).astype(jnp.bfloat16)

    def draw_gain(rng_key, shape):
        return 1.0 + 0.3 * jax.random.normal(rng_key, shape, jnp.float32)

    cache_shape = (NUM_LAYERS, SEQ_COUNT, CACHE_LEN, KV_HEADS, HEAD_DIM)
    return dict(
        hidden=draw_normal(part_keys[0], (SEQ_COUNT, MODEL_DIM), 1.0),
        positions=draw_positions(part_keys[1]),
        expert_ids=draw_routes(part_keys[2]),
        k_cache=draw_normal(part_keys[3], cache_shape, 1.0),
        v_cache=draw_normal(part_keys[4], cache_shape, 1.0),
        w_query=draw_normal(shared[0], (NUM_LAYERS, MODEL_DIM, Q_WIDTH), MODEL_DIM ** -0.5),
        w_key=draw_normal(shared[1], (NUM_LAYERS, MODEL_DIM, KV_WIDTH), MODEL_DIM ** -0.5),
        w_value=draw_normal(shared[2], (NUM_LAYERS, MODEL_DIM, KV_WIDTH), MODEL_DIM ** -0.5),
        w_out=draw_normal(shared[3], (NUM_LAYERS, Q_WIDTH, MODEL_DIM), 2.0 * Q_WIDTH ** -0.5),
        attn_gain=draw_gain(shared[4], (NUM_LAYERS, MODEL_DIM)),
        q_gain=draw_gain(shared[5], (NUM_LAYERS, Q_WIDTH)),
        k_gain=draw_gain(shared[6], (NUM_LAYERS, KV_WIDTH)),
        mlp_gain=draw_gain(shared[7], (NUM_LAYERS, MODEL_DIM)),
        w_router=draw_normal(shared[8], (MODEL_DIM, NUM_EXPERTS), MODEL_DIM ** -0.5),
        w_gate=draw_normal(shared[9], (NUM_EXPERTS, MODEL_DIM, FFN_DIM), MODEL_DIM ** -0.5),
        w_up=draw_normal(shared[10], (NUM_EXPERTS, MODEL_DIM, FFN_DIM), MODEL_DIM ** -0.5),
        w_down=draw_normal(shared[11], (NUM_EXPERTS, FFN_DIM, MODEL_DIM), NUM_EXPERTS * TOP_K ** -0.5 * FFN_DIM ** -0.5),
    )


def rms_norm(values, gain_vec):
    values = values.astype(jnp.float32)
    inv_rms = lax.rsqrt(jnp.mean(values * values, axis=-1, keepdims=True) + RMS_EPS)
    return values * inv_rms * gain_vec.astype(jnp.float32)


def rope_rotate(values, positions):
    half_dim = values.shape[-1] // 2
    frequencies = ROPE_BASE ** (-jnp.arange(half_dim, dtype=jnp.float32) / half_dim)
    angles = positions.astype(jnp.float32)[:, None] * frequencies[None, :]
    angles = angles.reshape((angles.shape[0],) + (1,) * (values.ndim - 2) + (half_dim,))
    cosines = jnp.cos(angles)
    sines = jnp.sin(angles)
    first_half = values[..., :half_dim]
    second_half = values[..., half_dim:]
    return jnp.concatenate([first_half * cosines - second_half * sines, second_half * cosines + first_half * sines], axis=-1)


def attention_layer(hidden, positions, k_layer, v_layer, w_query, w_key, w_value, w_out, attn_gain, q_gain, k_gain):
    head_group = NUM_HEADS // KV_HEADS
    normed = rms_norm(hidden, attn_gain).astype(jnp.bfloat16)
    q_heads = rms_norm(jnp.dot(normed, w_query, preferred_element_type=jnp.float32), q_gain)
    key_row = rms_norm(jnp.dot(normed, w_key, preferred_element_type=jnp.float32), k_gain)
    value_row = jnp.dot(normed, w_value, preferred_element_type=jnp.float32).astype(jnp.bfloat16)
    value_row = value_row.reshape(SEQ_COUNT, KV_HEADS, HEAD_DIM)
    q_heads = rope_rotate(q_heads.reshape(SEQ_COUNT, KV_HEADS, head_group, HEAD_DIM), positions).astype(jnp.bfloat16)
    key_row = rope_rotate(key_row.reshape(SEQ_COUNT, KV_HEADS, HEAD_DIM), positions).astype(jnp.bfloat16)
    hit_mask = (jnp.arange(CACHE_LEN)[None, :] == positions[:, None])[:, :, None, None]
    k_layer = jnp.where(hit_mask, key_row[:, None], k_layer)
    v_layer = jnp.where(hit_mask, value_row[:, None], v_layer)
    scores = jnp.einsum('bkgd,bskd->bkgs', q_heads.astype(jnp.float32), k_layer.astype(jnp.float32)) * HEAD_DIM ** -0.5
    valid_mask = (jnp.arange(CACHE_LEN)[None, :] <= positions[:, None])[:, None, None, :]
    scores = jnp.where(valid_mask, scores, -1e30)
    prob_vals = jax.nn.softmax(scores, axis=-1).astype(jnp.bfloat16)
    mixed_out = jnp.einsum('bkgs,bskd->bkgd', prob_vals.astype(jnp.float32), v_layer.astype(jnp.float32))
    mixed_out = mixed_out.astype(jnp.bfloat16).reshape(SEQ_COUNT, Q_WIDTH)
    hidden = (hidden.astype(jnp.float32) + jnp.dot(mixed_out, w_out, preferred_element_type=jnp.float32)).astype(jnp.bfloat16)
    return hidden, k_layer, v_layer


def moe_layer(hidden, routes, mlp_gain, w_router, w_gate, w_up, w_down):
    normed = rms_norm(hidden, mlp_gain).astype(jnp.bfloat16)
    router_prob = jax.nn.softmax(jnp.dot(normed, w_router, preferred_element_type=jnp.float32), axis=-1)
    gate_vals = jnp.take_along_axis(router_prob, routes, axis=1)
    flat_ids = routes.reshape(-1)
    sort_order = jnp.argsort(flat_ids, stable=True)
    counts = jnp.sum(flat_ids[:, None] == jnp.arange(NUM_EXPERTS)[None, :], axis=0, dtype=jnp.int32)
    starts = jnp.cumsum(counts) - counts
    per_expert = EP_GROUPS * CAPACITY
    padded = jnp.concatenate([sort_order, jnp.zeros((per_expert,), sort_order.dtype)])

    def expert_rows(item_pair):
        expert, start_at = item_pair
        copies = lax.dynamic_slice(padded, (start_at,), (per_expert,))
        token_rows = normed[copies // TOP_K]
        gate_act = jnp.dot(token_rows, w_gate[expert], preferred_element_type=jnp.float32)
        up_act = jnp.dot(token_rows, w_up[expert], preferred_element_type=jnp.float32)
        hidden_act = (jax.nn.silu(gate_act) * up_act).astype(jnp.bfloat16)
        return jnp.dot(hidden_act, w_down[expert], preferred_element_type=jnp.float32).astype(jnp.bfloat16)

    outputs = lax.map(expert_rows, (jnp.arange(NUM_EXPERTS), starts))
    copy_rank = jnp.argsort(sort_order, stable=True)
    within = copy_rank - starts[flat_ids]
    picked = outputs[flat_ids, within].reshape(SEQ_COUNT, TOP_K, MODEL_DIM)
    moe_out = jnp.sum(gate_vals[:, :, None] * picked.astype(jnp.float32), axis=1)
    return (hidden.astype(jnp.float32) + moe_out).astype(jnp.bfloat16)


def reference(hidden, positions, expert_ids, k_cache, v_cache, w_query, w_key, w_value, w_out, attn_gain, q_gain, k_gain, mlp_gain, w_router, w_gate, w_up, w_down):
    k_layers = []
    v_layers = []
    for layer_idx in range(NUM_LAYERS):
        hidden, k_layer, v_layer = attention_layer(hidden, positions, k_cache[layer_idx], v_cache[layer_idx], w_query[layer_idx], w_key[layer_idx], w_value[layer_idx], w_out[layer_idx], attn_gain[layer_idx], q_gain[layer_idx], k_gain[layer_idx])
        k_layers.append(k_layer)
        v_layers.append(v_layer)
        hidden = moe_layer(hidden, expert_ids[layer_idx], mlp_gain[layer_idx], w_router, w_gate, w_up, w_down)
    return hidden, jnp.stack(k_layers), jnp.stack(v_layers)
```

```python
import functools

import jax
import jax.numpy as jnp
import numpy as np
from jax import lax
from jax.experimental import pallas as pl
from jax.experimental.pallas import tpu as pltpu
from jax.sharding import PartitionSpec as P

MESH = pl.DeviceIdType.MESH
F32 = jnp.float32
BF16 = jnp.bfloat16
RMS_EPS = 1e-5
ROPE_BASE = 10000.0
CB = 512
SLOTS = 15


def rms_scale(v):
    return lax.rsqrt(jnp.mean(v * v, axis=-1, keepdims=True) + RMS_EPS)


def dot(a, b):
    return jnp.dot(a, b, preferred_element_type=F32)


def dot_t0(a, b):
    return lax.dot_general(a, b, (((0,), (0,)), ((), ())), preferred_element_type=F32)


def step_kernel(dims, hid, pos, ids, kc, vc, wq, wk, wv, wo, ag, qg, kg, mg, wr, wg, wu, wd, ctab, stab,
                out, kn, vn,
                ring, rsem, ssem, posv, idsv, agv, qgv, kgv, mgv, ctv, stv, xcur, hbuf, qf, kf, vf, mx,
                kcv, vcv, posb, cosb, sinb, rk, xg, xd, act, yb, cb, part, prt, far, comb, near, wrv, knb, vnb,
                rkss, rkrs, agss, agrs, rsss, rsrs, osem):
    n_layers, n_ep, T, D, QW, KVW, HD, S, E, EL, F, CAP = dims
    KV = KVW // HD
    H = QW // HD
    HG = H // KV
    NX = n_ep // 2
    NCH = D // CB
    NQ = QW // CB
    NO = NCH * (QW // D)
    NGU = 3 * EL
    ND1 = EL * F // D
    ND = NCH * ND1
    O_AT = NQ + 2
    G_AT = O_AT + NO
    D_AT = G_AT + NGU
    TOT = D_AT + ND
    CF = F - CB

    me = lax.axis_index("ep")
    core = lax.rem(me, 2)
    chip = me // 2
    sgn = 1 - 2 * core
    nchip = lax.rem(chip + sgn + NX, NX)
    pchip = lax.rem(chip - sgn + NX, NX)
    ochip = lax.rem(chip + 2, NX)
    partner = me + sgn
    nxt = nchip * 2 + core
    prv = pchip * 2 + core
    opp = ochip * 2 + core

    def slot_rows(k):
        return pl.ds(pl.multiple_of(lax.rem(k, SLOTS) * D, D), D)

    def issue(k):
        @pl.when(k < n_layers * TOT)
        def _():
            l = k // TOT
            r = lax.rem(k, TOT)
            s = lax.rem(k, SLOTS)
            dst = ring.at[slot_rows(k)]
            sem = rsem.at[s]

            def cols(i):
                return pl.ds(pl.multiple_of(i * CB, CB), CB)

            @pl.when(r < NQ)
            def _():
                pltpu.make_async_copy(wq.at[l, :, cols(r)], dst, sem).start()

            @pl.when(r == NQ)
            def _():
                pltpu.make_async_copy(wk.at[l], dst, sem).start()

            @pl.when(r == NQ + 1)
            def _():
                pltpu.make_async_copy(wv.at[l], dst, sem).start()

            @pl.when((r >= O_AT) & (r < G_AT))
            def _():
                j = r - O_AT
                half = lax.rem(j, QW // D)
                rows = pl.ds(pl.multiple_of(half * D, D), D)
                pltpu.make_async_copy(wo.at[l, rows, cols(j // (QW // D))], dst, sem).start()

            @pl.when((r >= G_AT) & (r < D_AT))
            def _():
                j = r - G_AT
                e = j // 3
                piece = lax.rem(j, 3)

                @pl.when(piece == 0)
                def _():
                    pltpu.make_async_copy(wg.at[e, :, 0:CB], dst, sem).start()

                @pl.when(piece == 1)
                def _():
                    pltpu.make_async_copy(wu.at[e, :, 0:CB], dst, sem).start()

                @pl.when(piece == 2)
                def _():
                    pltpu.make_async_copy(wg.at[e, :, CB:F], ring.at[slot_rows(k), 0:CF], sem).start()
                    pltpu.make_async_copy(wu.at[e, :, CB:F], ring.at[slot_rows(k), CF:CB], sem).start()

            @pl.when(r >= D_AT)
            def _():
                j = r - D_AT
                rows = pl.ds(pl.multiple_of(lax.rem(j, ND1) * D, D), D)
                pltpu.make_async_copy(wd.at[rows, cols(j // ND1)], dst, sem).start()

    def arrive(k):
        pltpu.make_async_copy(wk.at[0], ring.at[slot_rows(k)], rsem.at[lax.rem(k, SLOTS)]).wait()

    smalls = ((hid, xcur), (pos, posv), (ids, idsv), (ag, agv), (qg, qgv), (kg, kgv), (mg, mgv), (ctab, ctv), (stab, stv))
    small_copies = [pltpu.make_async_copy(a, b, ssem.at[i]) for i, (a, b) in enumerate(smalls)]
    for cp in small_copies:
        cp.start()

    def prime(k, carry):
        issue(k)
        return carry

    lax.fori_loop(0, SLOTS, prime, 0)
    big_copies = [pltpu.make_async_copy(a, b, ssem.at[len(smalls) + i]) for i, (a, b) in enumerate(((kc, kcv), (vc, vcv), (wr, wrv)))]
    for cp in big_copies:
        cp.start()

    barrier = pltpu.get_barrier_semaphore()
    for dev in (partner, nxt, prv):
        pl.semaphore_signal(barrier, inc=1, device_id={"ep": dev}, device_id_type=MESH)
    for cp in small_copies:
        cp.wait()

    posf = jnp.broadcast_to(posv[...].astype(F32), (T, HD))
    posb[...] = posf
    cos = jnp.zeros((T, HD), F32)
    sin = jnp.zeros((T, HD), F32)
    for s in range(S):
        hit = posf == float(s)
        cos = jnp.where(hit, ctv[s:s + 1, :], cos)
        sin = jnp.where(hit, stv[s:s + 1, :], sin)
    cosb[...] = cos
    sinb[...] = sin

    lane_e = lax.broadcasted_iota(jnp.int32, (T, E), 1)
    tril = (lax.broadcasted_iota(jnp.int32, (T, T), 0) > lax.broadcasted_iota(jnp.int32, (T, T), 1))
    tril = jnp.where(tril, 1.0, 0.0).astype(BF16)
    for l in range(n_layers):
        idl = idsv[l]
        chosen = jnp.zeros((T, E), F32)
        for j in range(idl.shape[1]):
            chosen = jnp.where(idl[:, j:j + 1] == lane_e, 1.0, chosen)
        rank = dot(tril, chosen.astype(BF16))
        rk[me, :, l * E:(l + 1) * E] = jnp.where(chosen > 0.5, rank, -1.0).astype(BF16)

    pl.semaphore_wait(barrier, 3)

    def rcopy(src, dst, ss, rs, dev):
        return pltpu.make_async_remote_copy(src_ref=src, dst_ref=dst, send_sem=ss, recv_sem=rs, device_id={"ep": dev}, device_id_type=MESH)

    def gather_stages(view, ss, rs):
        def cp(block, kind, dev):
            return rcopy(view(block), view(block), ss(kind), rs(kind), dev)

        def own():
            cp(me, 0, partner).start()
            cp(me, 1, nxt).start()
            cp(me, 2, prv).start()

        def forward():
            cp(prv, 1, nxt).wait_recv()
            cp(prv, 3, nxt).start()
            cp(prv, 4, partner).start()
            cp(nxt, 2, prv).wait_recv()
            cp(nxt, 5, partner).start()

        def across():
            cp(opp, 3, nxt).wait_recv()
            cp(opp, 6, partner).start()

        def finish():
            for kind in (0, 4, 5, 6):
                cp(me, kind, partner).wait_recv()
            for kind in range(7):
                cp(me, kind, partner).wait_send()

        return own, forward, across, finish

    own, forward, across, finish = gather_stages(lambda b: rk.at[b], lambda i: rkss.at[i], lambda i: rkrs.at[i])
    own()
    forward()
    across()
    finish()

    for cp in big_copies:
        cp.wait()

    col = lax.broadcasted_iota(jnp.int32, (8, S * KV * 8), 1)
    col_b = col // (S * KV)
    col_s = lax.rem(col // KV, S).astype(F32)
    col_kv = lax.rem(col, KV)
    diag = col_b == lax.broadcasted_iota(jnp.int32, (8, S * KV * 8), 0)
    GR = 8 * S * KV

    def layer(l, carry):
        base = l * TOT
        x = xcur[...].astype(F32)
        hbuf[...] = (x * rms_scale(x) * agv[pl.ds(l, 1), :]).astype(BF16)

        def q_step(j, c):
            k = base + j
            arrive(k)
            qf[:, pl.ds(pl.multiple_of(j * CB, CB), CB)] = dot(hbuf[...], ring[slot_rows(k), :])
            issue(k + SLOTS)
            return c

        lax.fori_loop(0, NQ, q_step, 0)
        arrive(base + NQ)
        kf[...] = dot(hbuf[...], ring[slot_rows(base + NQ), :])
        issue(base + NQ + SLOTS)
        arrive(base + NQ + 1)
        vf[...] = dot(hbuf[...], ring[slot_rows(base + NQ + 1), :])
        issue(base + NQ + 1 + SLOTS)

        def attend(g, c):
            rows = pl.ds(pl.multiple_of(g * 8, 8), 8)
            crows = pl.ds(pl.multiple_of(g * GR, GR), GR)
            cos8 = cosb[rows, :]
            sin8 = sinb[rows, :]
            pos8 = posb[rows, :]

            def rope(t):
                return t * cos8 + pltpu.roll(t, HD // 2, 1) * sin8

            q8 = qf[rows, :]
            q8 = q8 * rms_scale(q8) * qgv[pl.ds(l, 1), :]
            qs = jnp.concatenate([rope(q8[:, h * HD:(h + 1) * HD]) for h in range(H)], axis=0).astype(BF16)
            k8 = kf[rows, :]
            k8 = k8 * rms_scale(k8) * kgv[pl.ds(l, 1), :]
            k_tiles = [rope(k8[:, h * HD:(h + 1) * HD]) for h in range(KV)]
            kf[rows, :] = jnp.concatenate(k_tiles, axis=1)
            v8 = vf[rows, :]
            v_tiles = [v8[:, h * HD:(h + 1) * HD] for h in range(KV)]
            fresh = jnp.concatenate([jnp.concatenate(k_tiles, axis=0), jnp.concatenate(v_tiles, axis=0), jnp.ones((8 * KV, HD), F32)], axis=1).astype(BF16)
            posw = jnp.concatenate([pos8] * (GR // HD), axis=1)
            hit8 = diag & (col_s == posw)
            ok8 = diag & (col_s <= posw)
            place = jnp.concatenate([jnp.where(hit8 & (col_kv == h), 1.0, 0.0) for h in range(KV)], axis=0).astype(BF16)
            okay = jnp.concatenate([jnp.where(ok8 & (col_kv == h), 1.0, 0.0)[None, None] for h in range(KV)], axis=0)
            put = dot_t0(place, fresh)
            hits = put[:, 2 * HD:] > 0.5
            kb = jnp.where(hits, put[:, :HD], kcv[l, crows, :].astype(F32)).astype(BF16)
            vb = jnp.where(hits, put[:, HD:2 * HD], vcv[l, crows, :].astype(F32)).astype(BF16)
            sc = lax.dot_general(qs, kb, (((1,), (1,)), ((), ())), preferred_element_type=F32) * (HD ** -0.5)
            sc = sc.reshape(KV, HG, 8, GR)
            sc = jnp.where(jnp.broadcast_to(okay, sc.shape) > 0.5, sc, -1e30).reshape(H * 8, GR)
            ex = jnp.exp(sc - jnp.max(sc, axis=-1, keepdims=True))
            pr = (ex * (1.0 / jnp.sum(ex, axis=-1, keepdims=True))).astype(BF16)
            mixed = dot(pr, vb)
            qf[rows, :] = jnp.concatenate([mixed[h * 8:(h + 1) * 8, :] for h in range(H)], axis=1)
            return c

        lax.fori_loop(0, T // 8, attend, 0)
        mx[...] = qf[...].astype(BF16)

        @pl.when(l > 0)
        def _():
            pltpu.make_async_copy(knb, kn.at[0], osem.at[0]).wait()
            pltpu.make_async_copy(vnb, vn.at[0], osem.at[1]).wait()

        knb[...] = kf[...].astype(BF16)
        vnb[...] = vf[...].astype(BF16)
        pltpu.make_async_copy(knb, kn.at[l], osem.at[0]).start()
        pltpu.make_async_copy(vnb, vn.at[l], osem.at[1]).start()

        stages = []
        for n in range(NCH):
            cs = slice(n * CB, (n + 1) * CB)
            stages.append(gather_stages(lambda b, cs=cs: xg.at[b, :, cs], lambda i, n=n: agss.at[n, i], lambda i, n=n: agrs.at[n, i]))
        for n in range(NCH):
            cs = slice(n * CB, (n + 1) * CB)
            acc = xcur[:, cs].astype(F32)
            total = None
            for half in range(QW // D):
                k = base + O_AT + n * (QW // D) + half
                arrive(k)
                term = dot(mx[:, half * D:(half + 1) * D], ring[slot_rows(k), :])
                total = term if total is None else total + term
                issue(k + SLOTS)
            xn = (acc + total).astype(BF16)
            xcur[:, cs] = xn
            xg[me, :, cs] = xn
            stages[n][0]()
            if n >= 1:
                stages[n - 1][1]()
            if n >= 2:
                stages[n - 2][2]()
        stages[NCH - 1][1]()
        stages[NCH - 2][2]()
        stages[NCH - 1][2]()
        for n in range(NCH):
            stages[n][3]()

        lane = lax.broadcasted_iota(jnp.int32, (E, EL * 2 * CAP), 1)
        expand = jnp.where(lax.broadcasted_iota(jnp.int32, (E, EL * 2 * CAP), 0) == me * EL + lane // (2 * CAP), 1.0, 0.0).astype(BF16)
        lane_t = lax.broadcasted_iota(jnp.int32, (2 * T, EL * 2 * CAP), 1)
        same = lax.rem(lane_t // CAP, 2) == lax.broadcasted_iota(jnp.int32, (2 * T, EL * 2 * CAP), 0) // T
        lane_c = lax.rem(lane_t, CAP).astype(F32)
        lcol = pl.ds(pl.multiple_of(l * E, E), E)

        def route(xc, c):
            xp = xg[pl.ds(xc * 2, 2)].reshape(2 * T, D).astype(F32)
            hp = (xp * rms_scale(xp) * mgv[pl.ds(l, 1), :]).astype(BF16)
            logits = dot(hp, wrv[...])
            ex = jnp.exp(logits - jnp.max(logits, axis=-1, keepdims=True))
            prob = ex * (1.0 / jnp.sum(ex, axis=-1, keepdims=True))
            ranks = dot(rk[pl.ds(xc * 2, 2), :, lcol].reshape(2 * T, E), expand)
            pick = same & (ranks == lane_c)
            g1 = prob.astype(BF16)
            r1 = prob - g1.astype(F32)
            g2 = r1.astype(BF16)
            g3 = (r1 - g2.astype(F32)).astype(BF16)
            for i, gpart in enumerate((g1, g2, g3)):
                cb[xc, i * 2 * T:(i + 1) * 2 * T, :] = jnp.where(pick, dot(gpart, expand), 0.0).astype(BF16)
            onehot = jnp.where(pick, 1.0, 0.0).astype(BF16)
            for n in range(NCH):
                rows = dot_t0(onehot, hp[:, n * CB:(n + 1) * CB]).astype(BF16)
                xd[:, pl.ds(pl.multiple_of(xc * 2 * CAP, 2 * CAP), 2 * CAP), n * CB:(n + 1) * CB] = rows.reshape(EL, 2 * CAP, CB)
            return c

        lax.fori_loop(0, NX, route, 0)

        def gate_up(e, c):
            k = base + G_AT + 3 * e
            xe = xd[e]
            arrive(k)
            ga = dot(xe, ring[slot_rows(k), :])
            issue(k + SLOTS)
            arrive(k + 1)
            up = dot(xe, ring[slot_rows(k + 1), :])
            issue(k + 1 + SLOTS)
            act[e, :, 0:CB] = (jax.nn.silu(ga) * up).astype(BF16)
            arrive(k + 2)
            gu = dot(xe, ring[slot_rows(k + 2), :])
            issue(k + 2 + SLOTS)
            act[e, :, CB:F] = (jax.nn.silu(gu[:, :CF]) * gu[:, CF:]).astype(BF16)
            return c

        lax.fori_loop(0, EL, gate_up, 0)

        def send0(n):
            return rcopy(part.at[n, 1 - core], prt.at[n], rsss.at[n, 0], rsrs.at[n, 0], partner)

        def send_far(n):
            return rcopy(part.at[n, core, ochip], far.at[n], rsss.at[n, 1], rsrs.at[n, 1], nxt)

        def send_near(n):
            return rcopy(part.at[n, core, pchip], near.at[n], rsss.at[n, 2], rsrs.at[n, 2], prv)

        def send_comb(n):
            return rcopy(part.at[n, core, nchip], comb.at[n], rsss.at[n, 3], rsrs.at[n, 3], nxt)

        def stage1(n):
            send0(n).wait_recv()
            part[n, core] = part[n, core] + prt[n]
            send_far(n).start()
            send_near(n).start()

        def stage2(n):
            send_far(n).wait_recv()
            part[n, core, nchip] = part[n, core, nchip] + far[n]
            send_comb(n).start()

        def stage3(n):
            send_near(n).wait_recv()
            send_comb(n).wait_recv()
            cs = pl.ds(pl.multiple_of(n * CB, CB), CB)
            total = part[n, core, chip] + comb[n] + near[n]
            xcur[:, cs] = (xcur[:, cs].astype(F32) + total).astype(BF16)

        def down(n, c):
            def piece(i, cc):
                k = base + D_AT + n * ND1 + 3 * i
                for j in range(3):
                    arrive(k + j)
                row0 = lax.rem(k, SLOTS) * D
                per = 3 * D // F
                for m in range(per):
                    e = i * per + m
                    wrows = pl.ds(pl.multiple_of(row0 + m * F, 256), F)
                    y = dot(act[e], ring[wrows, :]).astype(BF16)
                    for xc in range(NX):
                        yb[xc, pl.ds(pl.multiple_of(e * 2 * CAP, 2 * CAP), 2 * CAP), :] = y[xc * 2 * CAP:(xc + 1) * 2 * CAP, :]
                for j in range(3):
                    issue(k + j + SLOTS)
                return cc

            lax.fori_loop(0, ND1 // 3, piece, 0)
            for xc in range(NX):
                p3 = dot(cb[xc], yb[xc])
                p1 = p3[:2 * T] + (p3[2 * T:4 * T] + p3[4 * T:])
                part[n, 0, xc] = p1[:T]
                part[n, 1, xc] = p1[T:]
            send0(n).start()

            @pl.when(n >= 1)
            def _():
                stage1(n - 1)

            @pl.when(n >= 2)
            def _():
                stage2(n - 2)

            @pl.when(n >= 3)
            def _():
                stage3(n - 3)

            return c

        lax.fori_loop(0, NCH, down, 0)
        stage1(NCH - 1)
        stage2(NCH - 2)
        stage3(NCH - 3)
        stage2(NCH - 1)
        stage3(NCH - 2)
        stage3(NCH - 1)

        def drain(n, c):
            send0(n).wait_send()
            send_far(n).wait_send()
            send_near(n).wait_send()
            send_comb(n).wait_send()
            return c

        lax.fori_loop(0, NCH, drain, 0)
        return carry

    lax.fori_loop(0, n_layers, layer, 0)
    last = pltpu.make_async_copy(xcur, out, osem.at[2])
    last.start()
    pltpu.make_async_copy(knb, kn.at[0], osem.at[0]).wait()
    pltpu.make_async_copy(vnb, vn.at[0], osem.at[1]).wait()
    last.wait()


def rope_tables(cache_len, head_dim):
    half = head_dim // 2
    freq = np.float32(ROPE_BASE) ** (-np.arange(half, dtype=np.float32) / np.float32(half))
    ang = np.arange(cache_len, dtype=np.float32)[:, None] * freq.astype(np.float32)[None, :]
    cos = np.cos(ang).astype(np.float32)
    sin = np.sin(ang).astype(np.float32)
    return np.concatenate([cos, cos], axis=1), np.concatenate([-sin, sin], axis=1)


def solution(mesh):
    n_ep = mesh.shape['ep']
    batch_axes = ('dp', 'ep')

    def device_step(hidden, positions, expert_ids, k_cache, v_cache, w_query, w_key, w_value, w_out, attn_gain, q_gain, k_gain, mlp_gain, w_router, w_gate, w_up, w_down):
        L, T, top_k = expert_ids.shape
        D = hidden.shape[1]
        S, KV, HD = k_cache.shape[2:]
        QW = w_query.shape[2]
        KVW = w_key.shape[2]
        E = w_router.shape[1]
        EL, _, F = w_gate.shape
        CAP = 2 * T * top_k // E
        NX = n_ep // 2
        NCH = D // CB
        dims = (L, n_ep, T, D, QW, KVW, HD, S, E, EL, F, CAP)
        ctab, stab = rope_tables(S, HD)
        rows = T * S * KV
        anyspec = pl.BlockSpec(memory_space=pl.ANY)
        V = pltpu.VMEM
        DMA = pltpu.SemaphoreType.DMA
        scratch = [
            V((SLOTS * D, CB), BF16), DMA((SLOTS,)), DMA((12,)),
            V((T, 1), jnp.int32), V((L, T, top_k), jnp.int32),
            V((L, D), F32), V((L, QW), F32), V((L, KVW), F32), V((L, D), F32),
            V((S, HD), F32), V((S, HD), F32),
            V((T, D), BF16), V((T, D), BF16), V((T, QW), F32), V((T, KVW), F32), V((T, KVW), F32), V((T, QW), BF16),
            V((L, rows, HD), BF16), V((L, rows, HD), BF16),
            V((T, HD), F32), V((T, HD), F32), V((T, HD), F32),
            V((n_ep, T, L * E), BF16), V((n_ep, T, D), BF16),
            V((EL, n_ep * CAP, D), BF16), V((EL, n_ep * CAP, F), BF16),
            V((NX, EL * 2 * CAP, CB), BF16), V((NX, 6 * T, EL * 2 * CAP), BF16),
            V((NCH, 2, NX, T, CB), F32), V((NCH, NX, T, CB), F32),
            V((NCH, T, CB), F32), V((NCH, T, CB), F32), V((NCH, T, CB), F32),
            V((D, E), BF16), V((T, KVW), BF16), V((T, KVW), BF16),
            DMA((7,)), DMA((7,)), DMA((NCH, 7)), DMA((NCH, 7)), DMA((NCH, 4)), DMA((NCH, 4)), DMA((3,)),
        ]
        out, kn, vn = pl.pallas_call(
            functools.partial(step_kernel, dims),
            out_shape=(jax.ShapeDtypeStruct((T, D), BF16), jax.ShapeDtypeStruct((L, T, KVW), BF16), jax.ShapeDtypeStruct((L, T, KVW), BF16)),
            in_specs=[anyspec] * 19,
            out_specs=(anyspec,) * 3,
            scratch_shapes=scratch,
            compiler_params=pltpu.CompilerParams(collective_id=0, has_side_effects=True, vmem_limit_bytes=67043328),
            name="moe_decode",
        )(hidden, positions.reshape(T, 1), expert_ids, k_cache.reshape(L, rows, HD), v_cache.reshape(L, rows, HD),
          w_query, w_key, w_value, w_out, attn_gain, q_gain, k_gain, mlp_gain, w_router, w_gate, w_up,
          w_down.reshape(EL * F, D), jnp.asarray(ctab), jnp.asarray(stab))
        hit = (jnp.arange(S)[None, :] == positions[:, None])[None, :, :, None, None]
        k_new = jnp.where(hit, kn.reshape(L, T, 1, KV, HD), k_cache)
        v_new = jnp.where(hit, vn.reshape(L, T, 1, KV, HD), v_cache)
        return out, k_new, v_new

    row_spec = P(batch_axes, None)
    cache_spec = P(None, batch_axes, None, None, None)
    full_spec = P()
    expert_spec = P('ep', None, None)
    in_specs = (row_spec, P(batch_axes), P(None, batch_axes, None), cache_spec, cache_spec, full_spec, full_spec, full_spec, full_spec, full_spec, full_spec, full_spec, full_spec, full_spec, expert_spec, expert_spec, expert_spec)
    return jax.shard_map(device_step, mesh=mesh, in_specs=in_specs, out_specs=(row_spec, cache_spec, cache_spec), check_vma=False)
```

```python
import functools

import jax
import jax.numpy as jnp
import numpy as np
from jax import lax
from jax.experimental import pallas as pl
from jax.experimental.pallas import tpu as pltpu
from jax.sharding import PartitionSpec as P

MESH = pl.DeviceIdType.MESH
F32 = jnp.float32
BF16 = jnp.bfloat16
RMS_EPS = 1e-5
ROPE_BASE = 10000.0
CB = 512
SLOTS = 18
PAIR = 2


def rms_scale(v):
    return lax.rsqrt(jnp.mean(v * v, axis=-1, keepdims=True) + RMS_EPS)


def dot(a, b):
    return jnp.dot(a, b, preferred_element_type=F32)


def dot_t1(a, b):
    return lax.dot_general(a, b, (((1,), (1,)), ((), ())), preferred_element_type=F32)


def dot_t0(a, b):
    return lax.dot_general(a, b, (((0,), (0,)), ((), ())), preferred_element_type=F32)


def step_kernel(dims, hid, pos, ids, kc, vc, wq, wk, wv, wo, ag, qg, kg, mg, wr, wg, wu, wd, ctab, stab,
                out, ko, vo,
                ring, rsem, ssem, posv, idsv, agv, qgv, kgv, mgv, ctv, stv, xcur, hbuf, qf, kf, vf, mf,
                kcv, vcv, posb, cosb, sinb, rk, xg, xd, act, yb, cb, part, prt, far, comb, near, wrv,
                rkss, rkrs, agss, agrs, rsss, rsrs, osem):
    n_layers, n_ep, T, D, QW, KVW, HD, S, E, EL, F, CAP = dims
    KV = KVW // HD
    H = QW // HD
    HG = H // KV
    NX = n_ep // 2
    NCH = D // CB
    NQ = QW // CB
    NO = NCH * (QW // D)
    NGU = 3 * EL
    ND1 = EL * F // D
    ND = NCH * ND1
    O_AT = NQ + 2
    G_AT = O_AT + NO
    D_AT = G_AT + NGU
    TOT = D_AT + ND
    CF = F - CB

    me = lax.axis_index("ep")
    core = lax.rem(me, 2)
    chip = me // 2
    sgn = 1 - 2 * core
    nchip = lax.rem(chip + sgn + NX, NX)
    pchip = lax.rem(chip - sgn + NX, NX)
    ochip = lax.rem(chip + 2, NX)
    partner = me + sgn
    nxt = nchip * 2 + core
    prv = pchip * 2 + core
    opp = ochip * 2 + core

    def slot_rows(k):
        return pl.ds(pl.multiple_of(lax.rem(k, SLOTS) * D, D), D)

    def issue(k):
        @pl.when(k < n_layers * TOT)
        def _():
            l = k // TOT
            r = lax.rem(k, TOT)
            s = lax.rem(k, SLOTS)
            dst = ring.at[slot_rows(k)]
            sem = rsem.at[s]

            def cols(i):
                return pl.ds(pl.multiple_of(i * CB, CB), CB)

            @pl.when(r < NQ)
            def _():
                pltpu.make_async_copy(wq.at[l, :, cols(r)], dst, sem).start(priority=1)

            @pl.when(r == NQ)
            def _():
                pltpu.make_async_copy(wk.at[l], dst, sem).start(priority=1)

            @pl.when(r == NQ + 1)
            def _():
                pltpu.make_async_copy(wv.at[l], dst, sem).start(priority=1)

            @pl.when((r >= O_AT) & (r < G_AT))
            def _():
                j = r - O_AT
                half = lax.rem(j, QW // D)
                rows = pl.ds(pl.multiple_of(half * D, D), D)
                pltpu.make_async_copy(wo.at[l, rows, cols(j // (QW // D))], dst, sem).start(priority=1)

            @pl.when((r >= G_AT) & (r < D_AT))
            def _():
                j = r - G_AT
                e = j // 3
                piece = lax.rem(j, 3)

                @pl.when(piece == 0)
                def _():
                    pltpu.make_async_copy(wg.at[e, :, 0:CB], dst, sem).start(priority=1)

                @pl.when(piece == 1)
                def _():
                    pltpu.make_async_copy(wu.at[e, :, 0:CB], dst, sem).start(priority=1)

                @pl.when(piece == 2)
                def _():
                    pltpu.make_async_copy(wg.at[e, :, CB:F], ring.at[slot_rows(k), 0:CF], sem).start(priority=1)
                    pltpu.make_async_copy(wu.at[e, :, CB:F], ring.at[slot_rows(k), CF:CB], sem).start(priority=1)

            @pl.when(r >= D_AT)
            def _():
                j = r - D_AT
                rows = pl.ds(pl.multiple_of(lax.rem(j, ND1) * D, D), D)
                pltpu.make_async_copy(wd.at[rows, cols(j // ND1)], dst, sem).start(priority=1)

    def arrive(k):
        pltpu.make_async_copy(wk.at[0], ring.at[slot_rows(k)], rsem.at[lax.rem(k, SLOTS)]).wait()

    smalls = ((hid, xcur), (pos, posv), (ids, idsv), (ag, agv), (qg, qgv), (kg, kgv), (mg, mgv), (ctab, ctv), (stab, stv))
    small_copies = [pltpu.make_async_copy(a, b, ssem.at[i]) for i, (a, b) in enumerate(smalls)]
    for cp in small_copies:
        cp.start()

    def prime(k, carry):
        issue(k)
        return carry

    lax.fori_loop(0, SLOTS, prime, 0)
    big_copies = [pltpu.make_async_copy(a, b, ssem.at[len(smalls) + i]) for i, (a, b) in enumerate(((kc, kcv), (vc, vcv), (wr, wrv)))]
    for cp in big_copies:
        cp.start()

    barrier = pltpu.get_barrier_semaphore()
    for dev in (partner, nxt, prv):
        pl.semaphore_signal(barrier, inc=1, device_id={"ep": dev}, device_id_type=MESH)
    for cp in small_copies:
        cp.wait()

    eye = lax.broadcasted_iota(jnp.int32, (T, T), 0) == lax.broadcasted_iota(jnp.int32, (T, T), 1)
    posc = jnp.sum(jnp.where(eye, jnp.broadcast_to(posv[...].astype(F32), (T, T)), 0.0), axis=1, keepdims=True)
    posf = jnp.broadcast_to(posc, (T, HD))
    posb[...] = posf
    cos = jnp.zeros((T, HD), F32)
    sin = jnp.zeros((T, HD), F32)
    for s in range(S):
        hit = posf == float(s)
        cos = jnp.where(hit, ctv[s:s + 1, :], cos)
        sin = jnp.where(hit, stv[s:s + 1, :], sin)
    cosb[...] = cos
    sinb[...] = sin

    row_e = lax.broadcasted_iota(jnp.int32, (E, T), 0)
    earlier = lax.broadcasted_iota(jnp.int32, (T, T), 0) < lax.broadcasted_iota(jnp.int32, (T, T), 1)
    earlier = jnp.where(earlier, 1.0, 0.0).astype(BF16)
    eye = jnp.where(eye, 1.0, 0.0).astype(BF16)
    for l in range(n_layers):
        idl = idsv[l]
        chosen = jnp.zeros((E, T), F32)
        for j in range(idl.shape[0]):
            chosen = jnp.where(idl[j:j + 1, :] == row_e, 1.0, chosen)
        rank = dot(chosen.astype(BF16), earlier)
        rank = jnp.where(chosen > 0.5, rank, -1.0).astype(BF16)
        rk[me, :, l * E:(l + 1) * E] = dot_t1(eye, rank).astype(BF16)

    pl.semaphore_wait(barrier, 3)

    def rcopy(src, dst, ss, rs, dev):
        return pltpu.make_async_remote_copy(src_ref=src, dst_ref=dst, send_sem=ss, recv_sem=rs, device_id={"ep": dev}, device_id_type=MESH)

    def gather_stages(view, ss, rs):
        def cp(block, kind, dev):
            return rcopy(view(block), view(block), ss(kind), rs(kind), dev)

        def own():
            cp(me, 0, partner).start()
            cp(me, 1, nxt).start()
            cp(me, 2, prv).start()

        def forward():
            cp(prv, 1, nxt).wait_recv()
            cp(prv, 3, nxt).start()
            cp(prv, 4, partner).start()
            cp(nxt, 2, prv).wait_recv()
            cp(nxt, 5, partner).start()

        def across():
            cp(opp, 3, nxt).wait_recv()
            cp(opp, 6, partner).start()

        def landed(kind):
            cp(me, kind, partner).wait_recv()

        def sent():
            for kind in range(7):
                cp(me, kind, partner).wait_send()

        return own, forward, across, landed, sent

    rk_own, rk_forward, rk_across, rk_landed, rk_sent = gather_stages(lambda b: rk.at[b], lambda i: rkss.at[i], lambda i: rkrs.at[i])
    rk_own()

    for cp in big_copies:
        cp.wait()

    col = lax.broadcasted_iota(jnp.int32, (8, S * KV * 8), 1)
    col_b = col // (S * KV)
    col_s = lax.rem(col // KV, S).astype(F32)
    col_kv = lax.rem(col, KV)
    diag = col_b == lax.broadcasted_iota(jnp.int32, (8, S * KV * 8), 0)
    GR = 8 * S * KV

    def layer(l, carry):
        base = l * TOT
        x = xcur[...].astype(F32)
        hbuf[...] = (x * rms_scale(x) * agv[pl.ds(l, 1), :]).astype(BF16)

        def q_step(j, c):
            k = base + j
            arrive(k)
            qf[:, pl.ds(pl.multiple_of(j * CB, CB), CB)] = dot(hbuf[...], ring[slot_rows(k), :])
            issue(k + SLOTS)
            return c

        lax.fori_loop(0, NQ, q_step, 0)
        arrive(base + NQ)
        kf[...] = dot(hbuf[...], ring[slot_rows(base + NQ), :])
        issue(base + NQ + SLOTS)
        arrive(base + NQ + 1)
        vf[...] = dot(hbuf[...], ring[slot_rows(base + NQ + 1), :])
        issue(base + NQ + 1 + SLOTS)

        @pl.when(l == 0)
        def _():
            rk_forward()

        def attend(i, c):
            groups = [i * PAIR + u for u in range(PAIR)]
            rows = [pl.ds(pl.multiple_of(g * 8, 8), 8) for g in groups]
            crows = [pl.ds(pl.multiple_of(g * GR, GR), GR) for g in groups]
            loads = [(qf[r, :], kf[r, :], vf[r, :], cosb[r, :], sinb[r, :], posb[r, :], kcv[l, cr, :], vcv[l, cr, :]) for r, cr in zip(rows, crows)]
            qgain = qgv[pl.ds(l, 1), :]
            kgain = kgv[pl.ds(l, 1), :]
            done = []
            for q8, k8, v8, cos8, sin8, pos8, kold, vold in loads:
                def rope(t):
                    return t * cos8 + pltpu.roll(t, HD // 2, 1) * sin8

                q8 = q8 * rms_scale(q8) * qgain
                qs = jnp.concatenate([rope(q8[:, h * HD:(h + 1) * HD]) for h in range(H)], axis=0).astype(BF16)
                k8 = k8 * rms_scale(k8) * kgain
                k_tiles = [rope(k8[:, h * HD:(h + 1) * HD]) for h in range(KV)]
                v_tiles = [v8[:, h * HD:(h + 1) * HD] for h in range(KV)]
                fresh = jnp.concatenate([jnp.concatenate(k_tiles, axis=0), jnp.concatenate(v_tiles, axis=0), jnp.ones((8 * KV, HD), F32)], axis=1).astype(BF16)
                posw = jnp.concatenate([pos8] * (GR // HD), axis=1)
                hit8 = diag & (col_s == posw)
                ok8 = diag & (col_s <= posw)
                place = jnp.concatenate([jnp.where(hit8 & (col_kv == h), 1.0, 0.0) for h in range(KV)], axis=0).astype(BF16)
                put = dot_t0(place, fresh)
                hits = put[:, 2 * HD:] > 0.5
                kb = jnp.where(hits, put[:, :HD], kold.astype(F32)).astype(BF16)
                vb = jnp.where(hits, put[:, HD:2 * HD], vold.astype(F32)).astype(BF16)
                sc = dot_t1(qs, kb)
                parts = []
                for h in range(KV):
                    okay = jnp.where(ok8 & (col_kv == h), 1.0, 0.0)[None]
                    sh = sc[h * HG * 8:(h + 1) * HG * 8].reshape(HG, 8, GR)
                    sh = jnp.where(jnp.broadcast_to(okay, sh.shape) > 0.5, sh * (HD ** -0.5), -1e30).reshape(HG * 8, GR)
                    ex = jnp.exp(sh - jnp.max(sh, axis=-1, keepdims=True))
                    parts.append((ex * (1.0 / jnp.sum(ex, axis=-1, keepdims=True))).astype(BF16))
                mixed = dot(jnp.concatenate(parts, axis=0), vb)
                done.append((jnp.concatenate([mixed[h * 8:(h + 1) * 8, :] for h in range(H)], axis=1), kb, vb))
            for r, cr, (m8, kb, vb) in zip(rows, crows, done):
                mf[r, :] = m8
                kcv[l, cr, :] = kb
                vcv[l, cr, :] = vb
            return c

        lax.fori_loop(0, T // 8 // PAIR, attend, 0)
        pltpu.make_async_copy(kcv.at[l], ko.at[l], osem.at[l, 0]).start()
        pltpu.make_async_copy(vcv.at[l], vo.at[l], osem.at[l, 1]).start()

        @pl.when(l == 0)
        def _():
            rk_across()

        stages = []
        for n in range(NCH):
            cs = slice(n * CB, (n + 1) * CB)
            stages.append(gather_stages(lambda b, cs=cs: xg.at[b, :, cs], lambda i, n=n: agss.at[n, i], lambda i, n=n: agrs.at[n, i]))
        for n in range(NCH):
            cs = slice(n * CB, (n + 1) * CB)
            acc = xcur[:, cs].astype(F32)
            total = None
            for half in range(QW // D):
                k = base + O_AT + n * (QW // D) + half
                arrive(k)
                term = dot(mf[:, half * D:(half + 1) * D].astype(BF16), ring[slot_rows(k), :])
                total = term if total is None else total + term
                issue(k + SLOTS)
            xn = (acc + total).astype(BF16)
            xcur[:, cs] = xn
            xg[me, :, cs] = xn
            stages[n][0]()
            if n >= 1:
                stages[n - 1][1]()
            if n >= 2:
                stages[n - 2][2]()
        lane = lax.broadcasted_iota(jnp.int32, (E, EL * 2 * CAP), 1)
        expand = jnp.where(lax.broadcasted_iota(jnp.int32, (E, EL * 2 * CAP), 0) == me * EL + lane // (2 * CAP), 1.0, 0.0).astype(BF16)
        lane_t = lax.broadcasted_iota(jnp.int32, (2 * T, EL * 2 * CAP), 1)
        same = lax.rem(lane_t // CAP, 2) == lax.broadcasted_iota(jnp.int32, (2 * T, EL * 2 * CAP), 0) // T
        lane_c = lax.rem(lane_t, CAP).astype(F32)
        lcol = pl.ds(pl.multiple_of(l * E, E), E)

        def route(i, c):
            @pl.when(i == 0)
            def _():
                for n in range(NCH):
                    stages[n][3](0)

                @pl.when(l == 0)
                def _():
                    for kind in (0, 4, 5, 6):
                        rk_landed(kind)
                    rk_sent()

            @pl.when(i == 1)
            def _():
                stages[NCH - 1][1]()
                for n in range(NCH):
                    stages[n][3](4)

            @pl.when(i == 2)
            def _():
                stages[NCH - 2][2]()
                for n in range(NCH):
                    stages[n][3](5)

            @pl.when(i == 3)
            def _():
                stages[NCH - 1][2]()
                for n in range(NCH):
                    stages[n][3](6)

            xc = jnp.where(i == 0, chip, jnp.where(i == 1, nchip, jnp.where(i == 2, pchip, ochip)))
            xp = xg[pl.ds(xc * 2, 2)].reshape(2 * T, D).astype(F32)
            hp = (xp * rms_scale(xp) * mgv[pl.ds(l, 1), :]).astype(BF16)
            logits = dot(hp, wrv[...])
            ex = jnp.exp(logits - jnp.max(logits, axis=-1, keepdims=True))
            prob = ex * (1.0 / jnp.sum(ex, axis=-1, keepdims=True))
            ranks = dot(rk[pl.ds(xc * 2, 2), :, lcol].reshape(2 * T, E), expand)
            pick = same & (ranks == lane_c)
            g1 = prob.astype(BF16)
            r1 = prob - g1.astype(F32)
            g2 = r1.astype(BF16)
            g3 = (r1 - g2.astype(F32)).astype(BF16)
            for i, gpart in enumerate((g1, g2, g3)):
                cb[xc, i * 2 * T:(i + 1) * 2 * T, :] = jnp.where(pick, dot(gpart, expand), 0.0).astype(BF16)
            onehot = jnp.where(pick, 1.0, 0.0).astype(BF16)
            for n in range(NCH):
                rows = dot_t0(onehot, hp[:, n * CB:(n + 1) * CB]).astype(BF16)
                xd[:, pl.ds(pl.multiple_of(xc * 2 * CAP, 2 * CAP), 2 * CAP), n * CB:(n + 1) * CB] = rows.reshape(EL, 2 * CAP, CB)
            return c

        lax.fori_loop(0, NX, route, 0)
        for n in range(NCH):
            stages[n][4]()

        def gate_up(e, c):
            k = base + G_AT + 3 * e
            xe = xd[e]
            arrive(k)
            ga = dot(xe, ring[slot_rows(k), :])
            issue(k + SLOTS)
            arrive(k + 1)
            up = dot(xe, ring[slot_rows(k + 1), :])
            issue(k + 1 + SLOTS)
            act[e, :, 0:CB] = (jax.nn.silu(ga) * up).astype(BF16)
            arrive(k + 2)
            gu = dot(xe, ring[slot_rows(k + 2), :])
            issue(k + 2 + SLOTS)
            act[e, :, CB:F] = (jax.nn.silu(gu[:, :CF]) * gu[:, CF:]).astype(BF16)
            return c

        lax.fori_loop(0, EL, gate_up, 0)

        def send0(n):
            return rcopy(part.at[n, 1 - core], prt.at[n], rsss.at[n, 0], rsrs.at[n, 0], partner)

        def send_far(n):
            return rcopy(part.at[n, core, ochip], far.at[n], rsss.at[n, 1], rsrs.at[n, 1], nxt)

        def send_near(n):
            return rcopy(part.at[n, core, pchip], near.at[n], rsss.at[n, 2], rsrs.at[n, 2], prv)

        def send_comb(n):
            return rcopy(part.at[n, core, nchip], comb.at[n], rsss.at[n, 3], rsrs.at[n, 3], nxt)

        def stage1(n):
            send0(n).wait_recv()
            part[n, core] = part[n, core] + prt[n]
            send_far(n).start()
            send_near(n).start()

        def stage2(n):
            send_far(n).wait_recv()
            part[n, core, nchip] = part[n, core, nchip] + far[n]
            send_comb(n).start()

        def stage3(n):
            send_near(n).wait_recv()
            send_comb(n).wait_recv()
            cs = pl.ds(pl.multiple_of(n * CB, CB), CB)
            total = part[n, core, chip] + comb[n] + near[n]
            xcur[:, cs] = (xcur[:, cs].astype(F32) + total).astype(BF16)

        def down(n, c):
            def piece(i, cc):
                k = base + D_AT + n * ND1 + 3 * i
                for j in range(3):
                    arrive(k + j)
                row0 = lax.rem(k, SLOTS) * D
                per = 3 * D // F
                for m in range(per):
                    e = i * per + m
                    wrows = pl.ds(pl.multiple_of(row0 + m * F, 256), F)
                    y = dot(act[e], ring[wrows, :]).astype(BF16)
                    for xc in range(NX):
                        yb[xc, pl.ds(pl.multiple_of(e * 2 * CAP, 2 * CAP), 2 * CAP), :] = y[xc * 2 * CAP:(xc + 1) * 2 * CAP, :]
                for j in range(3):
                    issue(k + j + SLOTS)
                return cc

            lax.fori_loop(0, ND1 // 3, piece, 0)
            for xc in range(NX):
                p3 = dot(cb[xc], yb[xc])
                p1 = p3[:2 * T] + (p3[2 * T:4 * T] + p3[4 * T:])
                part[n, 0, xc] = p1[:T]
                part[n, 1, xc] = p1[T:]
            send0(n).start()

            @pl.when(n >= 1)
            def _():
                stage1(n - 1)

            @pl.when(n >= 2)
            def _():
                stage2(n - 2)

            @pl.when(n >= 3)
            def _():
                stage3(n - 3)

            return c

        lax.fori_loop(0, NCH, down, 0)
        stage1(NCH - 1)
        stage2(NCH - 2)
        stage3(NCH - 3)
        stage2(NCH - 1)
        stage3(NCH - 2)
        stage3(NCH - 1)

        def drain(n, c):
            send0(n).wait_send()
            send_far(n).wait_send()
            send_near(n).wait_send()
            send_comb(n).wait_send()
            return c

        lax.fori_loop(0, NCH, drain, 0)
        return carry

    lax.fori_loop(0, n_layers, layer, 0)
    last = pltpu.make_async_copy(xcur, out, ssem.at[0])
    last.start()
    for l in range(n_layers):
        pltpu.make_async_copy(kcv.at[l], ko.at[l], osem.at[l, 0]).wait()
        pltpu.make_async_copy(vcv.at[l], vo.at[l], osem.at[l, 1]).wait()
    last.wait()


def rope_tables(cache_len, head_dim):
    half = head_dim // 2
    freq = np.float32(ROPE_BASE) ** (-np.arange(half, dtype=np.float32) / np.float32(half))
    ang = np.arange(cache_len, dtype=np.float32)[:, None] * freq.astype(np.float32)[None, :]
    cos = np.cos(ang).astype(np.float32)
    sin = np.sin(ang).astype(np.float32)
    return np.concatenate([cos, cos], axis=1), np.concatenate([-sin, sin], axis=1)


def solution(mesh):
    n_ep = mesh.shape['ep']
    batch_axes = ('dp', 'ep')

    def device_step(hidden, positions, expert_ids, k_cache, v_cache, w_query, w_key, w_value, w_out, attn_gain, q_gain, k_gain, mlp_gain, w_router, w_gate, w_up, w_down):
        L, T, top_k = expert_ids.shape
        D = hidden.shape[1]
        S, KV, HD = k_cache.shape[2:]
        QW = w_query.shape[2]
        KVW = w_key.shape[2]
        E = w_router.shape[1]
        EL, _, F = w_gate.shape
        CAP = 2 * T * top_k // E
        NX = n_ep // 2
        NCH = D // CB
        dims = (L, n_ep, T, D, QW, KVW, HD, S, E, EL, F, CAP)
        ctab, stab = rope_tables(S, HD)
        rows = T * S * KV
        anyspec = pl.BlockSpec(memory_space=pl.ANY)
        V = pltpu.VMEM
        DMA = pltpu.SemaphoreType.DMA
        scratch = [
            V((SLOTS * D, CB), BF16), DMA((SLOTS,)), DMA((12,)),
            V((1, T), jnp.int32), V((L, top_k, T), jnp.int32),
            V((L, D), F32), V((L, QW), F32), V((L, KVW), F32), V((L, D), F32),
            V((S, HD), F32), V((S, HD), F32),
            V((T, D), BF16), V((T, D), BF16), V((T, QW), F32), V((T, KVW), F32), V((T, KVW), F32), V((T, QW), F32),
            V((L, rows, HD), BF16), V((L, rows, HD), BF16),
            V((T, HD), F32), V((T, HD), F32), V((T, HD), F32),
            V((n_ep, T, L * E), BF16), V((n_ep, T, D), BF16),
            V((EL, n_ep * CAP, D), BF16), V((EL, n_ep * CAP, F), BF16),
            V((NX, EL * 2 * CAP, CB), BF16), V((NX, 6 * T, EL * 2 * CAP), BF16),
            V((NCH, 2, NX, T, CB), F32), V((NCH, NX, T, CB), F32),
            V((NCH, T, CB), F32), V((NCH, T, CB), F32), V((NCH, T, CB), F32),
            V((D, E), BF16),
            DMA((7,)), DMA((7,)), DMA((NCH, 7)), DMA((NCH, 7)), DMA((NCH, 4)), DMA((NCH, 4)), DMA((L, 2)),
        ]
        out, ko, vo = pl.pallas_call(
            functools.partial(step_kernel, dims),
            out_shape=(jax.ShapeDtypeStruct((T, D), BF16), jax.ShapeDtypeStruct((L, rows, HD), BF16), jax.ShapeDtypeStruct((L, rows, HD), BF16)),
            in_specs=[anyspec] * 19,
            out_specs=(anyspec,) * 3,
            scratch_shapes=scratch,
            compiler_params=pltpu.CompilerParams(collective_id=0, has_side_effects=True, vmem_limit_bytes=67043328),
            name="moe_decode",
        )(hidden, positions.reshape(1, T), expert_ids.transpose(0, 2, 1), k_cache.reshape(L, rows, HD), v_cache.reshape(L, rows, HD),
          w_query, w_key, w_value, w_out, attn_gain, q_gain, k_gain, mlp_gain, w_router, w_gate, w_up,
          w_down.reshape(EL * F, D), jnp.asarray(ctab), jnp.asarray(stab))
        return out, ko.reshape(k_cache.shape), vo.reshape(v_cache.shape)

    row_spec = P(batch_axes, None)
    cache_spec = P(None, batch_axes, None, None, None)
    full_spec = P()
    expert_spec = P('ep', None, None)
    in_specs = (row_spec, P(batch_axes), P(None, batch_axes, None), cache_spec, cache_spec, full_spec, full_spec, full_spec, full_spec, full_spec, full_spec, full_spec, full_spec, full_spec, expert_spec, expert_spec, expert_spec)
    return jax.shard_map(device_step, mesh=mesh, in_specs=in_specs, out_specs=(row_spec, cache_spec, cache_spec), check_vma=False)
```

```python
import functools

import jax
import jax.numpy as jnp
import numpy as np
from jax import lax
from jax.experimental import pallas as pl
from jax.experimental.pallas import tpu as pltpu
from jax.sharding import PartitionSpec as P

MESH = pl.DeviceIdType.MESH
F32 = jnp.float32
BF16 = jnp.bfloat16
RMS_EPS = 1e-5
ROPE_BASE = 10000.0
CB = 512
RB = 256
SLOTS = 18
PAIR = 4


def rms_scale(v):
    return lax.rsqrt(jnp.mean(v * v, axis=-1, keepdims=True) + RMS_EPS)


def dot(a, b):
    return jnp.dot(a, b, preferred_element_type=F32)


def dot_t1(a, b):
    return lax.dot_general(a, b, (((1,), (1,)), ((), ())), preferred_element_type=F32)


def dot_t0(a, b):
    return lax.dot_general(a, b, (((0,), (0,)), ((), ())), preferred_element_type=F32)


def step_kernel(dims, hid, pos, ids, kc, vc, wq, wk, wv, wo, ag, qg, kg, mg, wr, wg, wu, wd, ctab, stab,
                out, ko, vo,
                ring, rsem, ssem, posv, idsv, agv, qgv, kgv, mgv, ctv, stv, xcur, hbuf, qf, kf, vf, mf,
                kcv, vcv, posb, cosb, sinb, rk, xg, xd, act, yb, cb, part, prt, far, comb, near, wrv,
                rkss, rkrs, agss, agrs, rsss, rsrs, osem, csem):
    n_layers, n_ep, T, D, QW, KVW, HD, S, E, EL, F, CAP = dims
    KV = KVW // HD
    H = QW // HD
    HG = H // KV
    NX = n_ep // 2
    NCH = D // CB
    NQ = QW // CB
    NO = NCH * (QW // D)
    NGU = 3 * EL
    NR = D // RB
    ND1 = EL * F // (2 * D)
    ND = NR * ND1
    O_AT = NQ + 2
    G_AT = O_AT + NO
    D_AT = G_AT + NGU
    TOT = D_AT + ND
    CF = F - CB

    me = lax.axis_index("ep")
    core = lax.rem(me, 2)
    chip = me // 2
    sgn = 1 - 2 * core
    nchip = lax.rem(chip + sgn + NX, NX)
    pchip = lax.rem(chip - sgn + NX, NX)
    ochip = lax.rem(chip + 2, NX)
    partner = me + sgn
    nxt = nchip * 2 + core
    prv = pchip * 2 + core
    opp = ochip * 2 + core

    def slot_rows(k):
        return pl.ds(pl.multiple_of(lax.rem(k, SLOTS) * D, D), D)

    def issue(k):
        @pl.when(k < n_layers * TOT)
        def _():
            l = k // TOT
            r = lax.rem(k, TOT)
            s = lax.rem(k, SLOTS)
            dst = ring.at[slot_rows(k)]
            sem = rsem.at[s]

            def cols(i):
                return pl.ds(pl.multiple_of(i * CB, CB), CB)

            @pl.when(r < NQ)
            def _():
                pltpu.make_async_copy(wq.at[l, :, cols(r)], dst, sem).start(priority=1)

            @pl.when(r == NQ)
            def _():
                pltpu.make_async_copy(wk.at[l], dst, sem).start(priority=1)

            @pl.when(r == NQ + 1)
            def _():
                pltpu.make_async_copy(wv.at[l], dst, sem).start(priority=1)

            @pl.when((r >= O_AT) & (r < G_AT))
            def _():
                j = r - O_AT
                half = lax.rem(j, QW // D)
                rows = pl.ds(pl.multiple_of(half * D, D), D)
                pltpu.make_async_copy(wo.at[l, rows, cols(j // (QW // D))], dst, sem).start(priority=1)

            @pl.when((r >= G_AT) & (r < D_AT))
            def _():
                j = r - G_AT
                e = j // 3
                piece = lax.rem(j, 3)

                @pl.when(piece == 0)
                def _():
                    pltpu.make_async_copy(wg.at[e, :, 0:CB], dst, sem).start(priority=1)

                @pl.when(piece == 1)
                def _():
                    pltpu.make_async_copy(wu.at[e, :, 0:CB], dst, sem).start(priority=1)

                @pl.when(piece == 2)
                def _():
                    pltpu.make_async_copy(wg.at[e, :, CB:F], ring.at[slot_rows(k), 0:CF], sem).start(priority=1)
                    pltpu.make_async_copy(wu.at[e, :, CB:F], ring.at[slot_rows(k), CF:CB], sem).start(priority=1)

            @pl.when(r >= D_AT)
            def _():
                j = r - D_AT
                rcols = pl.ds(pl.multiple_of(j // ND1 * RB, RB), RB)
                for half in range(2):
                    rows = pl.ds(pl.multiple_of((half * ND1 + lax.rem(j, ND1)) * D, D), D)
                    pltpu.make_async_copy(wd.at[rows, rcols], ring.at[slot_rows(k), half * RB:(half + 1) * RB], sem).start(priority=1)

    def arrive(k):
        pltpu.make_async_copy(wk.at[0], ring.at[slot_rows(k)], rsem.at[lax.rem(k, SLOTS)]).wait()

    smalls = ((hid, xcur), (pos, posv), (ids, idsv), (ag, agv), (qg, qgv), (kg, kgv), (mg, mgv), (ctab, ctv), (stab, stv))
    small_copies = [pltpu.make_async_copy(a, b, ssem.at[i]) for i, (a, b) in enumerate(smalls)]
    for cp in small_copies:
        cp.start()

    def prime(k, carry):
        issue(k)
        return carry

    def cache_copies(l):
        return (pltpu.make_async_copy(kc.at[l], kcv.at[l], csem.at[l, 0]), pltpu.make_async_copy(vc.at[l], vcv.at[l], csem.at[l, 1]))

    router_copy = pltpu.make_async_copy(wr, wrv, ssem.at[len(smalls)])
    lax.fori_loop(0, O_AT, prime, 0)
    for cp in cache_copies(0):
        cp.start()
    router_copy.start()
    lax.fori_loop(O_AT, SLOTS, prime, 0)
    for l in range(1, n_layers):
        for cp in cache_copies(l):
            cp.start()

    barrier = pltpu.get_barrier_semaphore()
    for dev in (partner, nxt, prv):
        pl.semaphore_signal(barrier, inc=1, device_id={"ep": dev}, device_id_type=MESH)
    for cp in small_copies:
        cp.wait()

    eye = lax.broadcasted_iota(jnp.int32, (T, T), 0) == lax.broadcasted_iota(jnp.int32, (T, T), 1)
    posc = jnp.sum(jnp.where(eye, jnp.broadcast_to(posv[...].astype(F32), (T, T)), 0.0), axis=1, keepdims=True)
    posf = jnp.broadcast_to(posc, (T, HD))
    posb[...] = posf
    cos = jnp.zeros((T, HD), F32)
    sin = jnp.zeros((T, HD), F32)
    for s in range(S):
        hit = posf == float(s)
        cos = jnp.where(hit, ctv[s:s + 1, :], cos)
        sin = jnp.where(hit, stv[s:s + 1, :], sin)
    cosb[...] = cos
    sinb[...] = sin

    row_e = lax.broadcasted_iota(jnp.int32, (E, T), 0)
    earlier = lax.broadcasted_iota(jnp.int32, (T, T), 0) < lax.broadcasted_iota(jnp.int32, (T, T), 1)
    earlier = jnp.where(earlier, 1.0, 0.0).astype(BF16)
    eye = jnp.where(eye, 1.0, 0.0).astype(BF16)
    for l in range(n_layers):
        idl = idsv[l]
        chosen = jnp.zeros((E, T), F32)
        for j in range(idl.shape[0]):
            chosen = jnp.where(idl[j:j + 1, :] == row_e, 1.0, chosen)
        rank = dot(chosen.astype(BF16), earlier)
        rank = jnp.where(chosen > 0.5, rank, -1.0).astype(BF16)
        rk[me, :, l * E:(l + 1) * E] = dot_t1(eye, rank).astype(BF16)

    pl.semaphore_wait(barrier, 3)

    def rcopy(src, dst, ss, rs, dev):
        return pltpu.make_async_remote_copy(src_ref=src, dst_ref=dst, send_sem=ss, recv_sem=rs, device_id={"ep": dev}, device_id_type=MESH)

    def gather_stages(view, ss, rs):
        def cp(block, kind, dev):
            return rcopy(view(block), view(block), ss(kind), rs(kind), dev)

        def own():
            cp(me, 0, partner).start()
            cp(me, 1, nxt).start()
            cp(me, 2, prv).start()

        def forward():
            cp(prv, 1, nxt).wait_recv()
            cp(prv, 3, nxt).start()
            cp(prv, 4, partner).start()
            cp(nxt, 2, prv).wait_recv()
            cp(nxt, 5, partner).start()

        def across():
            cp(opp, 3, nxt).wait_recv()
            cp(opp, 6, partner).start()

        def landed(kind):
            cp(me, kind, partner).wait_recv()

        def sent():
            for kind in range(7):
                cp(me, kind, partner).wait_send()

        return own, forward, across, landed, sent

    rk_own, rk_forward, rk_across, rk_landed, rk_sent = gather_stages(lambda b: rk.at[b], lambda i: rkss.at[i], lambda i: rkrs.at[i])
    rk_own()

    col = lax.broadcasted_iota(jnp.int32, (8, S * KV * 8), 1)
    col_b = col // (S * KV)
    col_s = lax.rem(col // KV, S).astype(F32)
    col_kv = lax.rem(col, KV)
    diag = col_b == lax.broadcasted_iota(jnp.int32, (8, S * KV * 8), 0)
    GR = 8 * S * KV

    def layer(l, carry):
        base = l * TOT
        x = xcur[...].astype(F32)
        hbuf[...] = (x * rms_scale(x) * agv[pl.ds(l, 1), :]).astype(BF16)

        def q_step(j, c):
            k = base + 2 * j
            arrive(k)
            arrive(k + 1)
            for u in range(2):
                qf[:, pl.ds(pl.multiple_of((2 * j + u) * CB, CB), CB)] = dot(hbuf[...], ring[slot_rows(k + u), :])
            issue(k + SLOTS)
            issue(k + 1 + SLOTS)
            return c

        lax.fori_loop(0, NQ // 2, q_step, 0)
        arrive(base + NQ)
        arrive(base + NQ + 1)
        kf[...] = dot(hbuf[...], ring[slot_rows(base + NQ), :])
        vf[...] = dot(hbuf[...], ring[slot_rows(base + NQ + 1), :])
        issue(base + NQ + SLOTS)
        issue(base + NQ + 1 + SLOTS)
        for cp in cache_copies(l):
            cp.wait()

        @pl.when(l == 0)
        def _():
            rk_forward()

        def attend(i, c):
            groups = [i * PAIR + u for u in range(PAIR)]
            rows = [pl.ds(pl.multiple_of(g * 8, 8), 8) for g in groups]
            crows = [pl.ds(pl.multiple_of(g * GR, GR), GR) for g in groups]
            loads = [(qf[r, :], kf[r, :], vf[r, :], cosb[r, :], sinb[r, :], posb[r, :], kcv[l, cr, :], vcv[l, cr, :]) for r, cr in zip(rows, crows)]
            qgain = qgv[pl.ds(l, 1), :]
            kgain = kgv[pl.ds(l, 1), :]
            done = []
            for q8, k8, v8, cos8, sin8, pos8, kold, vold in loads:
                def rope(t):
                    return t * cos8 + pltpu.roll(t, HD // 2, 1) * sin8

                q8 = q8 * rms_scale(q8) * qgain
                qs = jnp.concatenate([rope(q8[:, h * HD:(h + 1) * HD]) for h in range(H)], axis=0).astype(BF16)
                k8 = k8 * rms_scale(k8) * kgain
                k_tiles = [rope(k8[:, h * HD:(h + 1) * HD]) for h in range(KV)]
                v_tiles = [v8[:, h * HD:(h + 1) * HD] for h in range(KV)]
                fresh = jnp.concatenate([jnp.concatenate(k_tiles, axis=0), jnp.concatenate(v_tiles, axis=0), jnp.ones((8 * KV, HD), F32)], axis=1).astype(BF16)
                posw = jnp.concatenate([pos8] * (GR // HD), axis=1)
                hit8 = diag & (col_s == posw)
                ok8 = diag & (col_s <= posw)
                place = jnp.concatenate([jnp.where(hit8 & (col_kv == h), 1.0, 0.0) for h in range(KV)], axis=0).astype(BF16)
                put = dot_t0(place, fresh)
                hits = put[:, 2 * HD:] > 0.5
                kb = jnp.where(hits, put[:, :HD], kold.astype(F32)).astype(BF16)
                vb = jnp.where(hits, put[:, HD:2 * HD], vold.astype(F32)).astype(BF16)
                sc = dot_t1(qs, kb)
                parts = []
                for h in range(KV):
                    okay = jnp.where(ok8 & (col_kv == h), 1.0, 0.0)[None]
                    sh = sc[h * HG * 8:(h + 1) * HG * 8].reshape(HG, 8, GR)
                    sh = jnp.where(jnp.broadcast_to(okay, sh.shape) > 0.5, sh * (HD ** -0.5), -1e30).reshape(HG * 8, GR)
                    ex = jnp.exp(sh - jnp.max(sh, axis=-1, keepdims=True))
                    parts.append((ex * (1.0 / jnp.sum(ex, axis=-1, keepdims=True))).astype(BF16))
                mixed = dot(jnp.concatenate(parts, axis=0), vb)
                done.append((jnp.concatenate([mixed[h * 8:(h + 1) * 8, :] for h in range(H)], axis=1), kb, vb))
            for r, cr, (m8, kb, vb) in zip(rows, crows, done):
                mf[r, :] = m8
                kcv[l, cr, :] = kb
                vcv[l, cr, :] = vb
            return c

        lax.fori_loop(0, T // 8 // PAIR, attend, 0)
        pltpu.make_async_copy(kcv.at[l], ko.at[l], osem.at[l, 0]).start()
        pltpu.make_async_copy(vcv.at[l], vo.at[l], osem.at[l, 1]).start()

        @pl.when(l == 0)
        def _():
            rk_across()

        stages = []
        for n in range(NCH):
            cs = slice(n * CB, (n + 1) * CB)
            stages.append(gather_stages(lambda b, cs=cs: xg.at[b, :, cs], lambda i, n=n: agss.at[n, i], lambda i, n=n: agrs.at[n, i]))
        for n in range(NCH):
            cs = slice(n * CB, (n + 1) * CB)
            acc = xcur[:, cs].astype(F32)
            total = None
            for half in range(QW // D):
                arrive(base + O_AT + n * (QW // D) + half)
            for half in range(QW // D):
                k = base + O_AT + n * (QW // D) + half
                term = dot(mf[:, half * D:(half + 1) * D].astype(BF16), ring[slot_rows(k), :])
                total = term if total is None else total + term
                issue(k + SLOTS)
            xn = (acc + total).astype(BF16)
            xcur[:, cs] = xn
            xg[me, :, cs] = xn
            stages[n][0]()
            if n >= 1:
                stages[n - 1][1]()
            if n >= 2:
                stages[n - 2][2]()
        lane = lax.broadcasted_iota(jnp.int32, (E, EL * 2 * CAP), 1)
        expand = jnp.where(lax.broadcasted_iota(jnp.int32, (E, EL * 2 * CAP), 0) == me * EL + lane // (2 * CAP), 1.0, 0.0).astype(BF16)
        lane_t = lax.broadcasted_iota(jnp.int32, (2 * T, EL * 2 * CAP), 1)
        same = lax.rem(lane_t // CAP, 2) == lax.broadcasted_iota(jnp.int32, (2 * T, EL * 2 * CAP), 0) // T
        lane_c = lax.rem(lane_t, CAP).astype(F32)
        lcol = pl.ds(pl.multiple_of(l * E, E), E)

        def route(i, c):
            @pl.when(i == 0)
            def _():
                for n in range(NCH):
                    stages[n][3](0)

                @pl.when(l == 0)
                def _():
                    for kind in (0, 4, 5, 6):
                        rk_landed(kind)
                    rk_sent()
                    router_copy.wait()

            @pl.when(i == 1)
            def _():
                stages[NCH - 1][1]()
                for n in range(NCH):
                    stages[n][3](4)

            @pl.when(i == 2)
            def _():
                stages[NCH - 2][2]()
                for n in range(NCH):
                    stages[n][3](5)

            @pl.when(i == 3)
            def _():
                stages[NCH - 1][2]()
                for n in range(NCH):
                    stages[n][3](6)

            xc = jnp.where(i == 0, chip, jnp.where(i == 1, nchip, jnp.where(i == 2, pchip, ochip)))
            xp = xg[pl.ds(xc * 2, 2)].reshape(2 * T, D).astype(F32)
            hp = (xp * rms_scale(xp) * mgv[pl.ds(l, 1), :]).astype(BF16)
            logits = dot(hp, wrv[...])
            ex = jnp.exp(logits - jnp.max(logits, axis=-1, keepdims=True))
            prob = ex * (1.0 / jnp.sum(ex, axis=-1, keepdims=True))
            ranks = dot(rk[pl.ds(xc * 2, 2), :, lcol].reshape(2 * T, E), expand)
            pick = same & (ranks == lane_c)
            g1 = prob.astype(BF16)
            r1 = prob - g1.astype(F32)
            g2 = r1.astype(BF16)
            g3 = (r1 - g2.astype(F32)).astype(BF16)
            for i, gpart in enumerate((g1, g2, g3)):
                cb[xc, i * 2 * T:(i + 1) * 2 * T, :] = jnp.where(pick, dot(gpart, expand), 0.0).astype(BF16)
            onehot = jnp.where(pick, 1.0, 0.0).astype(BF16)
            for n in range(NCH):
                rows = dot_t0(onehot, hp[:, n * CB:(n + 1) * CB]).astype(BF16)
                xd[:, pl.ds(pl.multiple_of(xc * 2 * CAP, 2 * CAP), 2 * CAP), n * CB:(n + 1) * CB] = rows.reshape(EL, 2 * CAP, CB)
            return c

        lax.fori_loop(0, NX, route, 0)
        for n in range(NCH):
            stages[n][4]()

        def gate_up(e, c):
            k = base + G_AT + 3 * e
            xe = xd[e]
            arrive(k)
            ga = dot(xe, ring[slot_rows(k), :])
            issue(k + SLOTS)
            arrive(k + 1)
            up = dot(xe, ring[slot_rows(k + 1), :])
            issue(k + 1 + SLOTS)
            act[e, :, 0:CB] = (jax.nn.silu(ga) * up).astype(BF16)
            arrive(k + 2)
            gu = dot(xe, ring[slot_rows(k + 2), :])
            issue(k + 2 + SLOTS)
            act[e, :, CB:F] = (jax.nn.silu(gu[:, :CF]) * gu[:, CF:]).astype(BF16)
            return c

        lax.fori_loop(0, EL, gate_up, 0)

        def send0(n):
            return rcopy(part.at[n, 1 - core], prt.at[n], rsss.at[n, 0], rsrs.at[n, 0], partner)

        def send_far(n):
            return rcopy(part.at[n, core, ochip], far.at[n], rsss.at[n, 1], rsrs.at[n, 1], nxt)

        def send_near(n):
            return rcopy(part.at[n, core, pchip], near.at[n], rsss.at[n, 2], rsrs.at[n, 2], prv)

        def send_comb(n):
            return rcopy(part.at[n, core, nchip], comb.at[n], rsss.at[n, 3], rsrs.at[n, 3], nxt)

        def stage1(n):
            send0(n).wait_recv()
            part[n, core] = part[n, core] + prt[n]
            send_far(n).start()
            send_near(n).start()

        def stage2(n):
            send_far(n).wait_recv()
            part[n, core, nchip] = part[n, core, nchip] + far[n]
            send_comb(n).start()

        def stage3(n):
            send_near(n).wait_recv()
            send_comb(n).wait_recv()
            cs = pl.ds(pl.multiple_of(n * RB, RB), RB)
            total = part[n, core, chip] + comb[n] + near[n]
            xcur[:, cs] = (xcur[:, cs].astype(F32) + total).astype(BF16)

        def down(n, c):
            k = base + D_AT + ND1 * n
            for j in range(ND1):
                arrive(k + j)
            row0 = lax.rem(k, SLOTS) * D
            per = EL // 2
            for e in range(EL):
                wrows = pl.ds(pl.multiple_of(row0 + (e % per) * F, 256), F)
                y = dot(act[e], ring[wrows, e // per * RB:(e // per + 1) * RB]).astype(BF16)
                for xc in range(NX):
                    yb[xc, e * 2 * CAP:(e + 1) * 2 * CAP, :] = y[xc * 2 * CAP:(xc + 1) * 2 * CAP, :]
            for j in range(ND1):
                issue(k + j + SLOTS)
            for xc in range(NX):
                p3 = dot(cb[xc], yb[xc])
                p1 = p3[:2 * T] + (p3[2 * T:4 * T] + p3[4 * T:])
                part[n, 0, xc] = p1[:T]
                part[n, 1, xc] = p1[T:]
            send0(n).start()

            @pl.when(n >= 1)
            def _():
                stage1(n - 1)

            @pl.when(n >= 3)
            def _():
                stage2(n - 3)

            @pl.when(n >= 5)
            def _():
                stage3(n - 5)

            return c

        lax.fori_loop(0, NR, down, 0)
        stage1(NR - 1)

        def tail(n, c):
            @pl.when(n < NR)
            def _():
                stage2(n)

            @pl.when(n - 2 < NR)
            def _():
                stage3(n - 2)

            return c

        lax.fori_loop(NR - 3, NR + 2, tail, 0)

        def drain(n, c):
            send0(n).wait_send()
            send_far(n).wait_send()
            send_near(n).wait_send()
            send_comb(n).wait_send()
            return c

        lax.fori_loop(0, NR, drain, 0)
        return carry

    lax.fori_loop(0, n_layers, layer, 0)
    last = pltpu.make_async_copy(xcur, out, ssem.at[0])
    last.start()
    for l in range(n_layers):
        pltpu.make_async_copy(kcv.at[l], ko.at[l], osem.at[l, 0]).wait()
        pltpu.make_async_copy(vcv.at[l], vo.at[l], osem.at[l, 1]).wait()
    last.wait()


def hand_over(out_in, k_in, v_in, out, k_out, v_out, obuf, kbuf, vbuf, isem, osem):
    pieces = []
    for l in range(k_in.shape[0]):
        quarter = k_in.shape[1] // 4
        for q in range(4):
            rows = pl.ds(q * quarter, quarter)
            pieces.append((k_in.at[l, rows], kbuf.at[l, rows], k_out.at[l, rows]))
            pieces.append((v_in.at[l, rows], vbuf.at[l, rows], v_out.at[l, rows]))
    pieces.append((out_in, obuf, out))
    loads = [pltpu.make_async_copy(a, b, isem.at[i]) for i, (a, b, _) in enumerate(pieces)]
    stores = [pltpu.make_async_copy(b, c, osem.at[i]) for i, (_, b, c) in enumerate(pieces)]
    for cp in loads:
        cp.start()
    for ld, st in zip(loads, stores):
        ld.wait()
        st.start()
    for st in stores:
        st.wait()


def rope_tables(cache_len, head_dim):
    half = head_dim // 2
    freq = np.float32(ROPE_BASE) ** (-np.arange(half, dtype=np.float32) / np.float32(half))
    ang = np.arange(cache_len, dtype=np.float32)[:, None] * freq.astype(np.float32)[None, :]
    cos = np.cos(ang).astype(np.float32)
    sin = np.sin(ang).astype(np.float32)
    return np.concatenate([cos, cos], axis=1), np.concatenate([-sin, sin], axis=1)


def solution(mesh):
    n_ep = mesh.shape['ep']
    batch_axes = ('dp', 'ep')

    def device_step(hidden, positions, expert_ids, k_cache, v_cache, w_query, w_key, w_value, w_out, attn_gain, q_gain, k_gain, mlp_gain, w_router, w_gate, w_up, w_down):
        L, T, top_k = expert_ids.shape
        D = hidden.shape[1]
        S, KV, HD = k_cache.shape[2:]
        QW = w_query.shape[2]
        KVW = w_key.shape[2]
        E = w_router.shape[1]
        EL, _, F = w_gate.shape
        CAP = 2 * T * top_k // E
        NX = n_ep // 2
        NCH = D // CB
        dims = (L, n_ep, T, D, QW, KVW, HD, S, E, EL, F, CAP)
        ctab, stab = rope_tables(S, HD)
        rows = T * S * KV
        anyspec = pl.BlockSpec(memory_space=pl.ANY)
        V = pltpu.VMEM
        DMA = pltpu.SemaphoreType.DMA
        scratch = [
            V((SLOTS * D, CB), BF16), DMA((SLOTS,)), DMA((12,)),
            V((1, T), jnp.int32), V((L, top_k, T), jnp.int32),
            V((L, D), F32), V((L, QW), F32), V((L, KVW), F32), V((L, D), F32),
            V((S, HD), F32), V((S, HD), F32),
            V((T, D), BF16), V((T, D), BF16), V((T, QW), F32), V((T, KVW), F32), V((T, KVW), F32), V((T, QW), F32),
            V((L, rows, HD), BF16), V((L, rows, HD), BF16),
            V((T, HD), F32), V((T, HD), F32), V((T, HD), F32),
            V((n_ep, T, L * E), BF16), V((n_ep, T, D), BF16),
            V((EL, n_ep * CAP, D), BF16), V((EL, n_ep * CAP, F), BF16),
            V((NX, EL * 2 * CAP, RB), BF16), V((NX, 6 * T, EL * 2 * CAP), BF16),
            V((D // RB, 2, NX, T, RB), F32), V((D // RB, NX, T, RB), F32),
            V((D // RB, T, RB), F32), V((D // RB, T, RB), F32), V((D // RB, T, RB), F32),
            V((D, E), BF16),
            DMA((7,)), DMA((7,)), DMA((NCH, 7)), DMA((NCH, 7)), DMA((D // RB, 4)), DMA((D // RB, 4)), DMA((L, 2)), DMA((L, 2)),
        ]
        out, ko, vo = pl.pallas_call(
            functools.partial(step_kernel, dims),
            out_shape=(jax.ShapeDtypeStruct((T, D), BF16), jax.ShapeDtypeStruct((L, rows, HD), BF16), jax.ShapeDtypeStruct((L, rows, HD), BF16)),
            in_specs=[anyspec] * 19,
            out_specs=(anyspec,) * 3,
            scratch_shapes=scratch,
            compiler_params=pltpu.CompilerParams(collective_id=0, has_side_effects=True, vmem_limit_bytes=67043328),
            name="moe_decode",
        )(hidden, positions.reshape(1, T), expert_ids.transpose(0, 2, 1), k_cache.reshape(L, rows, HD), v_cache.reshape(L, rows, HD),
          w_query, w_key, w_value, w_out, attn_gain, q_gain, k_gain, mlp_gain, w_router, w_gate, w_up,
          w_down.reshape(EL * F, D), jnp.asarray(ctab), jnp.asarray(stab))
        out, ko, vo = pl.pallas_call(
            hand_over,
            out_shape=tuple(jax.ShapeDtypeStruct(a.shape, BF16) for a in (out, ko, vo)),
            in_specs=[anyspec] * 3,
            out_specs=(anyspec,) * 3,
            scratch_shapes=[V((T, D), BF16), V((L, rows, HD), BF16), V((L, rows, HD), BF16), DMA((17,)), DMA((17,))],
            name="hand_over",
        )(out, ko, vo)
        return out, ko.reshape(k_cache.shape), vo.reshape(v_cache.shape)

    row_spec = P(batch_axes, None)
    cache_spec = P(None, batch_axes, None, None, None)
    full_spec = P()
    expert_spec = P('ep', None, None)
    in_specs = (row_spec, P(batch_axes), P(None, batch_axes, None), cache_spec, cache_spec, full_spec, full_spec, full_spec, full_spec, full_spec, full_spec, full_spec, full_spec, full_spec, expert_spec, expert_spec, expert_spec)
    return jax.shard_map(device_step, mesh=mesh, in_specs=in_specs, out_specs=(row_spec, cache_spec, cache_spec), check_vma=False)
```

```python
import functools

import jax
import jax.numpy as jnp
import numpy as np
from jax import lax
from jax.experimental import pallas as pl
from jax.experimental.pallas import tpu as pltpu
from jax.sharding import PartitionSpec as P

MESH = pl.DeviceIdType.MESH
F32 = jnp.float32
BF16 = jnp.bfloat16
RMS_EPS = 1e-5
ROPE_BASE = 10000.0
CB = 512
RB = 256
SLOTS = 18
PAIR = 4
PIECES = 4


def rms_scale(v):
    return lax.rsqrt(jnp.mean(v * v, axis=-1, keepdims=True) + RMS_EPS)


def dot(a, b):
    return jnp.dot(a, b, preferred_element_type=F32)


def dot_t1(a, b):
    return lax.dot_general(a, b, (((1,), (1,)), ((), ())), preferred_element_type=F32)


def dot_t0(a, b):
    return lax.dot_general(a, b, (((0,), (0,)), ((), ())), preferred_element_type=F32)


def step_kernel(dims, hid, pos, ids, kc, vc, wq, wk, wv, wo, ag, qg, kg, mg, wr, wg, wu, wd, ctab, stab,
                out, kn, vn,
                ring, rsem, ssem, posv, idsv, agv, qgv, kgv, mgv, ctv, stv, xcur, hbuf, qf, kf, vf, knb, vnb,
                kcv, vcv, posb, cosb, sinb, rk, xg, xd, act, yb, cb, part, prt, far, comb, near, wrv,
                rkss, rkrs, agss, agrs, rsss, rsrs, osem, csem):
    n_layers, n_ep, T, D, QW, KVW, HD, S, E, EL, F, CAP = dims
    KV = KVW // HD
    H = QW // HD
    HG = H // KV
    NX = n_ep // 2
    NCH = D // CB
    NQ = QW // CB
    NO = NCH * (QW // D)
    NGU = 3 * EL
    NR = D // RB
    ND1 = EL * F // (2 * D)
    ND = NR * ND1
    O_AT = NQ + 2
    G_AT = O_AT + NO
    D_AT = G_AT + NGU
    TOT = D_AT + ND
    CF = F - CB

    me = lax.axis_index("ep")
    core = lax.rem(me, 2)
    chip = me // 2
    sgn = 1 - 2 * core
    nchip = lax.rem(chip + sgn + NX, NX)
    pchip = lax.rem(chip - sgn + NX, NX)
    ochip = lax.rem(chip + 2, NX)
    partner = me + sgn
    nxt = nchip * 2 + core
    prv = pchip * 2 + core
    opp = ochip * 2 + core

    def slot_rows(k):
        return pl.ds(pl.multiple_of(lax.rem(k, SLOTS) * D, D), D)

    def issue(k):
        @pl.when(k < n_layers * TOT)
        def _():
            l = k // TOT
            r = lax.rem(k, TOT)
            s = lax.rem(k, SLOTS)
            dst = ring.at[slot_rows(k)]
            sem = rsem.at[s]

            def cols(i):
                return pl.ds(pl.multiple_of(i * CB, CB), CB)

            @pl.when(r < NQ)
            def _():
                pltpu.make_async_copy(wq.at[l, :, cols(r)], dst, sem).start(priority=1)

            @pl.when(r == NQ)
            def _():
                pltpu.make_async_copy(wk.at[l], dst, sem).start(priority=1)

            @pl.when(r == NQ + 1)
            def _():
                pltpu.make_async_copy(wv.at[l], dst, sem).start(priority=1)

            @pl.when((r >= O_AT) & (r < G_AT))
            def _():
                j = r - O_AT
                half = lax.rem(j, QW // D)
                rows = pl.ds(pl.multiple_of(half * D, D), D)
                pltpu.make_async_copy(wo.at[l, rows, cols(j // (QW // D))], dst, sem).start(priority=1)

            @pl.when((r >= G_AT) & (r < D_AT))
            def _():
                j = r - G_AT
                e = j // 3
                piece = lax.rem(j, 3)

                @pl.when(piece == 0)
                def _():
                    pltpu.make_async_copy(wg.at[e, :, 0:CB], dst, sem).start(priority=1)

                @pl.when(piece == 1)
                def _():
                    pltpu.make_async_copy(wu.at[e, :, 0:CB], dst, sem).start(priority=1)

                @pl.when(piece == 2)
                def _():
                    pltpu.make_async_copy(wg.at[e, :, CB:F], ring.at[slot_rows(k), 0:CF], sem).start(priority=1)
                    pltpu.make_async_copy(wu.at[e, :, CB:F], ring.at[slot_rows(k), CF:CB], sem).start(priority=1)

            @pl.when(r >= D_AT)
            def _():
                j = r - D_AT
                rcols = pl.ds(pl.multiple_of(j // ND1 * RB, RB), RB)
                for half in range(2):
                    rows = pl.ds(pl.multiple_of((half * ND1 + lax.rem(j, ND1)) * D, D), D)
                    pltpu.make_async_copy(wd.at[rows, rcols], ring.at[slot_rows(k), half * RB:(half + 1) * RB], sem).start(priority=1)

    def arrive(k):
        pltpu.make_async_copy(wk.at[0], ring.at[slot_rows(k)], rsem.at[lax.rem(k, SLOTS)]).wait()

    smalls = ((hid, xcur), (pos, posv), (ids, idsv), (ag, agv), (qg, qgv), (kg, kgv), (mg, mgv), (ctab, ctv), (stab, stv))
    small_copies = [pltpu.make_async_copy(a, b, ssem.at[i]) for i, (a, b) in enumerate(smalls)]
    for cp in small_copies:
        cp.start()

    def prime(k, carry):
        issue(k)
        return carry

    def cache_copies(l):
        return (pltpu.make_async_copy(kc.at[l], kcv, csem.at[0]), pltpu.make_async_copy(vc.at[l], vcv, csem.at[1]))

    router_copy = pltpu.make_async_copy(wr, wrv, ssem.at[len(smalls)])
    lax.fori_loop(0, O_AT, prime, 0)
    for cp in cache_copies(0):
        cp.start()
    router_copy.start()
    lax.fori_loop(O_AT, SLOTS, prime, 0)
    barrier = pltpu.get_barrier_semaphore()
    for dev in (partner, nxt, prv):
        pl.semaphore_signal(barrier, inc=1, device_id={"ep": dev}, device_id_type=MESH)
    for cp in small_copies:
        cp.wait()

    eye = lax.broadcasted_iota(jnp.int32, (T, T), 0) == lax.broadcasted_iota(jnp.int32, (T, T), 1)
    posc = jnp.sum(jnp.where(eye, jnp.broadcast_to(posv[...].astype(F32), (T, T)), 0.0), axis=1, keepdims=True)
    posf = jnp.broadcast_to(posc, (T, HD))
    posb[...] = posf
    cos = jnp.zeros((T, HD), F32)
    sin = jnp.zeros((T, HD), F32)
    for s in range(S):
        hit = posf == float(s)
        cos = jnp.where(hit, ctv[s:s + 1, :], cos)
        sin = jnp.where(hit, stv[s:s + 1, :], sin)
    cosb[...] = cos
    sinb[...] = sin

    row_e = lax.broadcasted_iota(jnp.int32, (E, T), 0)
    earlier = lax.broadcasted_iota(jnp.int32, (T, T), 0) < lax.broadcasted_iota(jnp.int32, (T, T), 1)
    earlier = jnp.where(earlier, 1.0, 0.0).astype(BF16)
    eye = jnp.where(eye, 1.0, 0.0).astype(BF16)
    for l in range(n_layers):
        idl = idsv[l]
        chosen = jnp.zeros((E, T), F32)
        for j in range(idl.shape[0]):
            chosen = jnp.where(idl[j:j + 1, :] == row_e, 1.0, chosen)
        rank = dot(chosen.astype(BF16), earlier)
        rank = jnp.where(chosen > 0.5, rank, -1.0).astype(BF16)
        rk[me, :, l * E:(l + 1) * E] = dot_t1(eye, rank).astype(BF16)

    pl.semaphore_wait(barrier, 3)

    def rcopy(src, dst, ss, rs, dev):
        return pltpu.make_async_remote_copy(src_ref=src, dst_ref=dst, send_sem=ss, recv_sem=rs, device_id={"ep": dev}, device_id_type=MESH)

    def gather_stages(view, ss, rs):
        def cp(block, kind, dev):
            return rcopy(view(block), view(block), ss(kind), rs(kind), dev)

        def own():
            cp(me, 0, partner).start()
            cp(me, 1, nxt).start()
            cp(me, 2, prv).start()

        def forward():
            cp(prv, 1, nxt).wait_recv()
            cp(prv, 3, nxt).start()
            cp(prv, 4, partner).start()
            cp(nxt, 2, prv).wait_recv()
            cp(nxt, 5, partner).start()

        def across():
            cp(opp, 3, nxt).wait_recv()
            cp(opp, 6, partner).start()

        def landed(kind):
            cp(me, kind, partner).wait_recv()

        def sent():
            for kind in range(7):
                cp(me, kind, partner).wait_send()

        return own, forward, across, landed, sent

    rk_own, rk_forward, rk_across, rk_landed, rk_sent = gather_stages(lambda b: rk.at[b], lambda i: rkss.at[i], lambda i: rkrs.at[i])
    rk_own()

    col = lax.broadcasted_iota(jnp.int32, (8, S * KV * 8), 1)
    col_b = col // (S * KV)
    col_s = lax.rem(col // KV, S).astype(F32)
    col_kv = lax.rem(col, KV)
    diag = col_b == lax.broadcasted_iota(jnp.int32, (8, S * KV * 8), 0)
    GR = 8 * S * KV
    o_row = lax.broadcasted_iota(jnp.int32, (8 * KV, 8 * KV), 0)
    o_col = lax.broadcasted_iota(jnp.int32, (8 * KV, 8 * KV), 1)
    order = jnp.where((o_row // KV == lax.rem(o_col, 8)) & (lax.rem(o_row, KV) == o_col // 8), 1.0, 0.0).astype(BF16)

    def layer(l, carry):
        base = l * TOT
        x = xcur[...].astype(F32)
        hbuf[...] = (x * rms_scale(x) * agv[pl.ds(l, 1), :]).astype(BF16)

        def q_step(j, c):
            k = base + 2 * j
            arrive(k)
            arrive(k + 1)
            for u in range(2):
                qf[:, pl.ds(pl.multiple_of((2 * j + u) * CB, CB), CB)] = dot(hbuf[...], ring[slot_rows(k + u), :])
            issue(k + SLOTS)
            issue(k + 1 + SLOTS)
            return c

        lax.fori_loop(0, NQ // 2, q_step, 0)
        arrive(base + NQ)
        arrive(base + NQ + 1)
        kf[...] = dot(hbuf[...], ring[slot_rows(base + NQ), :])
        vf[...] = dot(hbuf[...], ring[slot_rows(base + NQ + 1), :])
        issue(base + NQ + SLOTS)
        issue(base + NQ + 1 + SLOTS)
        for cp in cache_copies(l):
            cp.wait()

        @pl.when(l == 0)
        def _():
            rk_forward()

        def attend(i, c):
            groups = [i * PAIR + u for u in range(PAIR)]
            rows = [pl.ds(pl.multiple_of(g * 8, 8), 8) for g in groups]
            crows = [pl.ds(pl.multiple_of(g * GR, GR), GR) for g in groups]
            nrows = [pl.ds(pl.multiple_of(g * 8 * KV, 8 * KV), 8 * KV) for g in groups]
            loads = [(qf[r, :], kf[r, :], vf[r, :], cosb[r, :], sinb[r, :], posb[r, :], kcv[cr, :], vcv[cr, :]) for r, cr in zip(rows, crows)]
            qgain = qgv[pl.ds(l, 1), :]
            kgain = kgv[pl.ds(l, 1), :]
            done = []
            for q8, k8, v8, cos8, sin8, pos8, kold, vold in loads:
                def rope(t):
                    return t * cos8 + pltpu.roll(t, HD // 2, 1) * sin8

                q8 = q8 * rms_scale(q8) * qgain
                qs = jnp.concatenate([rope(q8[:, h * HD:(h + 1) * HD]) for h in range(H)], axis=0).astype(BF16)
                k8 = k8 * rms_scale(k8) * kgain
                k_tiles = [rope(k8[:, h * HD:(h + 1) * HD]) for h in range(KV)]
                v_tiles = [v8[:, h * HD:(h + 1) * HD] for h in range(KV)]
                kall = jnp.concatenate(k_tiles, axis=0).astype(BF16)
                vall = jnp.concatenate(v_tiles, axis=0).astype(BF16)
                fresh = dot(order, jnp.concatenate([kall, vall], axis=1)).astype(BF16)
                kall = kall.astype(F32)
                vall = vall.astype(F32)
                posw = jnp.concatenate([pos8] * (GR // HD), axis=1)
                past8 = diag & (col_s < posw)
                sc = dot_t1(qs, kold)
                qsf = qs.astype(F32)
                parts = []
                adds = []
                for h in range(KV):
                    hr = slice(h * HG * 8, (h + 1) * HG * 8)
                    okay = jnp.where(past8 & (col_kv == h), 1.0, 0.0)[None]
                    sh = sc[hr].reshape(HG, 8, GR)
                    sh = jnp.where(jnp.broadcast_to(okay, sh.shape) > 0.5, sh * (HD ** -0.5), -1e30).reshape(HG * 8, GR)
                    knew = kall[h * 8:(h + 1) * 8][None]
                    vnew = vall[h * 8:(h + 1) * 8][None]
                    nh = jnp.sum(qsf[hr].reshape(HG, 8, HD) * knew, axis=-1, keepdims=True).reshape(HG * 8, 1) * (HD ** -0.5)
                    top = jnp.maximum(jnp.max(sh, axis=-1, keepdims=True), nh)
                    ex = jnp.exp(sh - top)
                    en = jnp.exp(nh - top)
                    inv = 1.0 / (jnp.sum(ex, axis=-1, keepdims=True) + en)
                    parts.append((ex * inv).astype(BF16))
                    pn = jnp.broadcast_to((en * inv).astype(BF16).astype(F32), (HG * 8, HD))
                    adds.append((pn.reshape(HG, 8, HD) * vnew).reshape(HG * 8, HD))
                mixed = dot(jnp.concatenate(parts, axis=0), vold) + jnp.concatenate(adds, axis=0)
                done.append((jnp.concatenate([mixed[h * 8:(h + 1) * 8, :] for h in range(H)], axis=1), fresh))
            for r, nr, (m8, fresh) in zip(rows, nrows, done):
                qf[r, :] = m8
                knb[l, nr, :] = fresh[:, :HD]
                vnb[l, nr, :] = fresh[:, HD:]
            return c

        lax.fori_loop(0, T // 8 // PAIR, attend, 0)
        pltpu.make_async_copy(knb.at[l], kn.at[l], osem.at[l, 0]).start()
        pltpu.make_async_copy(vnb.at[l], vn.at[l], osem.at[l, 1]).start()

        @pl.when(l + 1 < n_layers)
        def _():
            for cp in cache_copies(l + 1):
                cp.start()

        @pl.when(l == 0)
        def _():
            rk_across()

        stages = []
        for n in range(NCH):
            cs = slice(n * CB, (n + 1) * CB)
            stages.append(gather_stages(lambda b, cs=cs: xg.at[b, :, cs], lambda i, n=n: agss.at[n, i], lambda i, n=n: agrs.at[n, i]))
        for n in range(NCH):
            cs = slice(n * CB, (n + 1) * CB)
            acc = xcur[:, cs].astype(F32)
            total = None
            for half in range(QW // D):
                arrive(base + O_AT + n * (QW // D) + half)
            for half in range(QW // D):
                k = base + O_AT + n * (QW // D) + half
                term = dot(qf[:, half * D:(half + 1) * D].astype(BF16), ring[slot_rows(k), :])
                total = term if total is None else total + term
                issue(k + SLOTS)
            xn = (acc + total).astype(BF16)
            xcur[:, cs] = xn
            xg[me, :, cs] = xn
            stages[n][0]()
            if n >= 1:
                stages[n - 1][1]()
            if n >= 2:
                stages[n - 2][2]()
        lane = lax.broadcasted_iota(jnp.int32, (E, EL * 2 * CAP), 1)
        expand = jnp.where(lax.broadcasted_iota(jnp.int32, (E, EL * 2 * CAP), 0) == me * EL + lane // (2 * CAP), 1.0, 0.0).astype(BF16)
        lane_t = lax.broadcasted_iota(jnp.int32, (2 * T, EL * 2 * CAP), 1)
        same = lax.rem(lane_t // CAP, 2) == lax.broadcasted_iota(jnp.int32, (2 * T, EL * 2 * CAP), 0) // T
        lane_c = lax.rem(lane_t, CAP).astype(F32)
        lcol = pl.ds(pl.multiple_of(l * E, E), E)

        def route(i, c):
            @pl.when(i == 0)
            def _():
                for n in range(NCH):
                    stages[n][3](0)

                @pl.when(l == 0)
                def _():
                    for kind in (0, 4, 5, 6):
                        rk_landed(kind)
                    rk_sent()
                    router_copy.wait()

            @pl.when(i == 1)
            def _():
                stages[NCH - 1][1]()
                for n in range(NCH):
                    stages[n][3](4)

            @pl.when(i == 2)
            def _():
                stages[NCH - 2][2]()
                for n in range(NCH):
                    stages[n][3](5)

            @pl.when(i == 3)
            def _():
                stages[NCH - 1][2]()
                for n in range(NCH):
                    stages[n][3](6)

            xc = jnp.where(i == 0, chip, jnp.where(i == 1, nchip, jnp.where(i == 2, pchip, ochip)))
            xp = xg[pl.ds(xc * 2, 2)].reshape(2 * T, D).astype(F32)
            hp = (xp * rms_scale(xp) * mgv[pl.ds(l, 1), :]).astype(BF16)
            logits = dot(hp, wrv[...])
            ex = jnp.exp(logits - jnp.max(logits, axis=-1, keepdims=True))
            prob = ex * (1.0 / jnp.sum(ex, axis=-1, keepdims=True))
            ranks = dot(rk[pl.ds(xc * 2, 2), :, lcol].reshape(2 * T, E), expand)
            pick = same & (ranks == lane_c)
            g1 = prob.astype(BF16)
            r1 = prob - g1.astype(F32)
            g2 = r1.astype(BF16)
            g3 = (r1 - g2.astype(F32)).astype(BF16)
            for i, gpart in enumerate((g1, g2, g3)):
                cb[xc, i * 2 * T:(i + 1) * 2 * T, :] = jnp.where(pick, dot(gpart, expand), 0.0).astype(BF16)
            onehot = jnp.where(pick, 1.0, 0.0).astype(BF16)
            for n in range(NCH):
                rows = dot_t0(onehot, hp[:, n * CB:(n + 1) * CB]).astype(BF16)
                xd[:, pl.ds(pl.multiple_of(xc * 2 * CAP, 2 * CAP), 2 * CAP), n * CB:(n + 1) * CB] = rows.reshape(EL, 2 * CAP, CB)
            return c

        lax.fori_loop(0, NX, route, 0)
        for n in range(NCH):
            stages[n][4]()

        def gate_up(e, c):
            k = base + G_AT + 3 * e
            xe = xd[e]
            arrive(k)
            ga = dot(xe, ring[slot_rows(k), :])
            issue(k + SLOTS)
            arrive(k + 1)
            up = dot(xe, ring[slot_rows(k + 1), :])
            issue(k + 1 + SLOTS)
            act[e, :, 0:CB] = (jax.nn.silu(ga) * up).astype(BF16)
            arrive(k + 2)
            gu = dot(xe, ring[slot_rows(k + 2), :])
            issue(k + 2 + SLOTS)
            act[e, :, CB:F] = (jax.nn.silu(gu[:, :CF]) * gu[:, CF:]).astype(BF16)
            return c

        lax.fori_loop(0, EL, gate_up, 0)

        def send0(n):
            return rcopy(part.at[n, 1 - core], prt.at[n], rsss.at[n, 0], rsrs.at[n, 0], partner)

        def send_far(n):
            return rcopy(part.at[n, core, ochip], far.at[n], rsss.at[n, 1], rsrs.at[n, 1], nxt)

        def send_near(n):
            return rcopy(part.at[n, core, pchip], near.at[n], rsss.at[n, 2], rsrs.at[n, 2], prv)

        def send_comb(n):
            return rcopy(part.at[n, core, nchip], comb.at[n], rsss.at[n, 3], rsrs.at[n, 3], nxt)

        def stage1(n):
            send0(n).wait_recv()
            part[n, core] = part[n, core] + prt[n]
            send_far(n).start()
            send_near(n).start()

        def stage2(n):
            send_far(n).wait_recv()
            part[n, core, nchip] = part[n, core, nchip] + far[n]
            send_comb(n).start()

        def stage3(n):
            send_near(n).wait_recv()
            send_comb(n).wait_recv()
            cs = pl.ds(pl.multiple_of(n * RB, RB), RB)
            total = part[n, core, chip] + comb[n] + near[n]
            xcur[:, cs] = (xcur[:, cs].astype(F32) + total).astype(BF16)

        def down(n, c):
            k = base + D_AT + ND1 * n
            for j in range(ND1):
                arrive(k + j)
            row0 = lax.rem(k, SLOTS) * D
            per = EL // 2
            for e in range(EL):
                wrows = pl.ds(pl.multiple_of(row0 + (e % per) * F, 256), F)
                y = dot(act[e], ring[wrows, e // per * RB:(e // per + 1) * RB]).astype(BF16)
                for xc in range(NX):
                    yb[xc, e * 2 * CAP:(e + 1) * 2 * CAP, :] = y[xc * 2 * CAP:(xc + 1) * 2 * CAP, :]
            for j in range(ND1):
                issue(k + j + SLOTS)
            for xc in range(NX):
                p3 = dot(cb[xc], yb[xc])
                p1 = p3[:2 * T] + (p3[2 * T:4 * T] + p3[4 * T:])
                part[n, 0, xc] = p1[:T]
                part[n, 1, xc] = p1[T:]
            send0(n).start()

            @pl.when(n >= 1)
            def _():
                stage1(n - 1)

            @pl.when(n >= 3)
            def _():
                stage2(n - 3)

            @pl.when(n >= 5)
            def _():
                stage3(n - 5)

            return c

        lax.fori_loop(0, NR, down, 0)
        stage1(NR - 1)

        def tail(n, c):
            @pl.when(n < NR)
            def _():
                stage2(n)

            @pl.when(n - 2 < NR)
            def _():
                stage3(n - 2)

            return c

        lax.fori_loop(NR - 3, NR + 2, tail, 0)

        def drain(n, c):
            send0(n).wait_send()
            send_far(n).wait_send()
            send_near(n).wait_send()
            send_comb(n).wait_send()
            return c

        lax.fori_loop(0, NR, drain, 0)
        return carry

    lax.fori_loop(0, n_layers, layer, 0)
    last = pltpu.make_async_copy(xcur, out, ssem.at[0])
    last.start()
    for l in range(n_layers):
        pltpu.make_async_copy(knb.at[l], kn.at[l], osem.at[l, 0]).wait()
        pltpu.make_async_copy(vnb.at[l], vn.at[l], osem.at[l, 1]).wait()
    last.wait()


def hand_over(pos, out_in, k_in, v_in, k_fresh, v_fresh, out, k_out, v_out, obuf, kbuf, vbuf, knew, vnew, isem, osem):
    span = k_in.shape[1] // PIECES
    fresh = [pltpu.make_async_copy(k_fresh, knew, isem.at[0]), pltpu.make_async_copy(v_fresh, vnew, isem.at[1])]
    jobs = [(out_in, obuf, out, None)]
    for l in range(k_in.shape[0]):
        for q in range(PIECES):
            seqs = pl.ds(q * span, span)
            jobs.append((k_in.at[l, seqs], kbuf.at[l, seqs], k_out.at[l, seqs], (kbuf, knew, l, q)))
            jobs.append((v_in.at[l, seqs], vbuf.at[l, seqs], v_out.at[l, seqs], (vbuf, vnew, l, q)))
    loads = [pltpu.make_async_copy(a, b, isem.at[2 + i]) for i, (a, b, _, _) in enumerate(jobs)]
    stores = [pltpu.make_async_copy(b, c, osem.at[i]) for i, (_, b, c, _) in enumerate(jobs)]
    for cp in fresh + loads:
        cp.start()
    for cp in fresh:
        cp.wait()
    for ld, st, (_, _, _, patch) in zip(loads, stores, jobs):
        ld.wait()
        if patch is not None:
            buf, new, l, q = patch
            for b in range(q * span, (q + 1) * span):
                buf[l, b, pos[b]] = new[l, b]
        st.start()
    for st in stores:
        st.wait()


def rope_tables(cache_len, head_dim):
    half = head_dim // 2
    freq = np.float32(ROPE_BASE) ** (-np.arange(half, dtype=np.float32) / np.float32(half))
    ang = np.arange(cache_len, dtype=np.float32)[:, None] * freq.astype(np.float32)[None, :]
    cos = np.cos(ang).astype(np.float32)
    sin = np.sin(ang).astype(np.float32)
    return np.concatenate([cos, cos], axis=1), np.concatenate([-sin, sin], axis=1)


def solution(mesh):
    n_ep = mesh.shape['ep']
    batch_axes = ('dp', 'ep')

    def device_step(hidden, positions, expert_ids, k_cache, v_cache, w_query, w_key, w_value, w_out, attn_gain, q_gain, k_gain, mlp_gain, w_router, w_gate, w_up, w_down):
        L, T, top_k = expert_ids.shape
        D = hidden.shape[1]
        S, KV, HD = k_cache.shape[2:]
        QW = w_query.shape[2]
        KVW = w_key.shape[2]
        E = w_router.shape[1]
        EL, _, F = w_gate.shape
        CAP = 2 * T * top_k // E
        NX = n_ep // 2
        NCH = D // CB
        dims = (L, n_ep, T, D, QW, KVW, HD, S, E, EL, F, CAP)
        ctab, stab = rope_tables(S, HD)
        rows = T * S * KV
        anyspec = pl.BlockSpec(memory_space=pl.ANY)
        V = pltpu.VMEM
        DMA = pltpu.SemaphoreType.DMA
        scratch = [
            V((SLOTS * D, CB), BF16), DMA((SLOTS,)), DMA((12,)),
            V((1, T), jnp.int32), V((L, top_k, T), jnp.int32),
            V((L, D), F32), V((L, QW), F32), V((L, KVW), F32), V((L, D), F32),
            V((S, HD), F32), V((S, HD), F32),
            V((T, D), BF16), V((T, D), BF16), V((T, QW), F32), V((T, KVW), F32), V((T, KVW), F32), V((L, T * KV, HD), BF16), V((L, T * KV, HD), BF16),
            V((rows, HD), BF16), V((rows, HD), BF16),
            V((T, HD), F32), V((T, HD), F32), V((T, HD), F32),
            V((n_ep, T, L * E), BF16), V((n_ep, T, D), BF16),
            V((EL, n_ep * CAP, D), BF16), V((EL, n_ep * CAP, F), BF16),
            V((NX, EL * 2 * CAP, RB), BF16), V((NX, 6 * T, EL * 2 * CAP), BF16),
            V((D // RB, 2, NX, T, RB), F32), V((D // RB, NX, T, RB), F32),
            V((D // RB, T, RB), F32), V((D // RB, T, RB), F32), V((D // RB, T, RB), F32),
            V((D, E), BF16),
            DMA((7,)), DMA((7,)), DMA((NCH, 7)), DMA((NCH, 7)), DMA((D // RB, 4)), DMA((D // RB, 4)), DMA((L, 2)), DMA((2,)),
        ]
        out, kn, vn = pl.pallas_call(
            functools.partial(step_kernel, dims),
            out_shape=(jax.ShapeDtypeStruct((T, D), BF16), jax.ShapeDtypeStruct((L, T * KV, HD), BF16), jax.ShapeDtypeStruct((L, T * KV, HD), BF16)),
            in_specs=[anyspec] * 19,
            out_specs=(anyspec,) * 3,
            scratch_shapes=scratch,
            compiler_params=pltpu.CompilerParams(collective_id=0, has_side_effects=True, vmem_limit_bytes=67043328),
            name="moe_decode",
        )(hidden, positions.reshape(1, T), expert_ids.transpose(0, 2, 1), k_cache.reshape(L, rows, HD), v_cache.reshape(L, rows, HD),
          w_query, w_key, w_value, w_out, attn_gain, q_gain, k_gain, mlp_gain, w_router, w_gate, w_up,
          w_down.reshape(EL * F, D), jnp.asarray(ctab), jnp.asarray(stab))
        n_copies = 2 * L * PIECES + 3
        return pl.pallas_call(
            hand_over,
            out_shape=tuple(jax.ShapeDtypeStruct(a.shape, BF16) for a in (out, k_cache, v_cache)),
            in_specs=[pl.BlockSpec(memory_space=pltpu.SMEM)] + [anyspec] * 5,
            out_specs=(anyspec,) * 3,
            scratch_shapes=[V((T, D), BF16), V(k_cache.shape, BF16), V(v_cache.shape, BF16), V((L, T, KV, HD), BF16), V((L, T, KV, HD), BF16),
                            DMA((n_copies,)), DMA((n_copies,))],
            name="hand_over",
        )(positions, out, k_cache, v_cache, kn.reshape(L, T, KV, HD), vn.reshape(L, T, KV, HD))

    row_spec = P(batch_axes, None)
    cache_spec = P(None, batch_axes, None, None, None)
    full_spec = P()
    expert_spec = P('ep', None, None)
    in_specs = (row_spec, P(batch_axes), P(None, batch_axes, None), cache_spec, cache_spec, full_spec, full_spec, full_spec, full_spec, full_spec, full_spec, full_spec, full_spec, full_spec, expert_spec, expert_spec, expert_spec)
    return jax.shard_map(device_step, mesh=mesh, in_specs=in_specs, out_specs=(row_spec, cache_spec, cache_spec), check_vma=False)
```
